32 devices in a mesh: group: 2 (over y), ctx: 4 (over z), section: 2 (over x), rep: 2 (over core).
Axes of the slice: x: 2, y: 2, z: 4, core: 2. Of those that a mesh axis runs over, the one named last changes fastest.
Arguments:
- stream: bfloat16 [1024, 4096], P(('group', 'ctx'), ('section', 'rep')), parts along dimension 0, may hold values from -12 to 12
- query_proj: bfloat16 [1024, 4096], P(('group', 'ctx'), ('section', 'rep')), parts along dimension 0, may hold values from -105 to 105
- key_proj: bfloat16 [1024, 256], P(('group', 'ctx')), parts along dimension 0, may hold values from -4 to 4
- value_projected: bfloat16 [1024, 256], P(('group', 'ctx')), parts along dimension 0, may hold values from -6 to 6
- expert_ids: int32 [1024, 2], P(('group', 'ctx')), parts along dimension 0, may hold values from 0 to 3, all different within a row; in each aligned block of 128 rows (0 to 127, 128 to 255, ...) at most 80 rows name the same one
- expert_home: int32 [4], replicated, may hold values from 0 to 3, each once
- router: bfloat16 [4096, 4], P(('section', 'rep')), may hold values from -0.09375 to 0.09375
- norm_gain: bfloat16 [4096], P(('section', 'rep')), may hold values from 0.25 to 1.75
- w_gate: bfloat16 [4, 4096, 768], P('ctx', ('section', 'rep')), may hold values from -0.09375 to 0.09375
- w_up: bfloat16 [4, 4096, 768], P('ctx', ('section', 'rep')), may hold values from -0.09375 to 0.09375
- w_down: bfloat16 [4, 768, 4096], P('ctx', None, ('section', 'rep')), may hold values from -0.21875 to 0.21875
Outputs:
- result: bfloat16 [1024, 4096], P(('group', 'ctx'), ('section', 'rep')), parts along dimension 0
The draws below stay inside these ranges and needn't reach their ends.
There are 2 independent parts, one for each index of `group`. The reference program is written for one: setup_inputs(seed, part) draws one part's arguments, and reference() takes and returns one part's arrays. A program takes and returns all parts, laid end to end along the dimension named above; an argument that names none is the same for every part. Nothing has to cross between parts.
Inputs may be any that keep to these rules, and one draw needn't show every extreme that they name: `expert_ids`: in each token's row the 2 experts differ; within the 128 tokens of one index of ctx no expert is chosen more than 80 times. `expert_home`: each index of ctx holds exactly one expert.
All inputs are finite; a program needn't handle non-finite values.
Results may differ from the reference program's by a relative error of at most 0.0085.
Values may be sent and summed in bfloat16 or wider, within the bound.
A program may use at most 64 MiB of HBM per device.

```python
import math
import jax
import jax.numpy as jnp
import numpy as np
from jax import lax

D = 4096
HEAD_SIZE = 128
QUERY_HEADS = 32
KEY_VALUE_HEADS = 2
HID = 768
TOK_DEV = 128
EXPERTS = 4
TOP = 2
BLOCK_TOKENS = 512
CAP = 80
N_SECTION = 2
N_REP = 2


def drawn_pair(key):
    start_offset = jax.random.fold_in(key, 4242)
    key_sample = jnp.clip(jax.random.normal(jax.random.fold_in(start_offset, 1), (BLOCK_TOKENS, KEY_VALUE_HEADS, HEAD_SIZE), jnp.float32), -4.0, 4.0)
    query_sample = jnp.clip(jax.random.normal(jax.random.fold_in(start_offset, 2), (BLOCK_TOKENS, KEY_VALUE_HEADS, QUERY_HEADS // KEY_VALUE_HEADS, HEAD_SIZE), jnp.float32), -4.0, 4.0)
    return (query_sample.reshape(BLOCK_TOKENS, QUERY_HEADS * HEAD_SIZE), key_sample.reshape(BLOCK_TOKENS, KEY_VALUE_HEADS * HEAD_SIZE))


def draw_query_proj(key, part):
    return drawn_pair(key)[0].astype(jnp.bfloat16)


def draw_key_proj(key, part):
    return drawn_pair(key)[1].astype(jnp.bfloat16)


def draw_stream(key, part):
    start_offset = jax.random.fold_in(key, 777)
    column_scale = jnp.linspace(0.5, 1.5, D)
    values = jnp.clip(jax.random.normal(jax.random.fold_in(start_offset, 3), (BLOCK_TOKENS, D), jnp.float32), -6.0, 6.0)
    return (values * column_scale[None, :]).astype(jnp.bfloat16)


def level_of(own_key, extent, split, smallest, largest):
    def one(dim, shards_of):
        heights = jax.random.uniform(jax.random.fold_in(jax.random.fold_in(own_key, 6), dim), (shards_of,), jnp.float32, smallest / len(split), largest / len(split))
        return jnp.repeat(jnp.exp(heights), extent[dim] // shards_of).reshape((-1,) + (1,) * (len(extent) - dim - 1))

    factor_of = one(*split[0])
    for cut in split[1:]:
        factor_of = factor_of * one(*cut)
    return factor_of


def deal_out(rng, own, number, rows, number_of, top, most, slope):
    sequence = jax.random.permutation(rng, number_of)
    crowded, usual = load_shares(number_of, rows * top, most, slope, True), load_shares(number_of, rows * top, most, slope, False)
    places = jnp.arange(number_of)

    def named(sizes, offset_by):
        used = int((sizes > 0).sum())
        fixed = max(1, used // 4)
        passed = fixed + (places - fixed + offset_by * (used - fixed)) % max(1, number_of - fixed)
        return jnp.zeros((number_of,), jnp.int32).at[sequence[jnp.where(places < fixed, places, passed)]].set(jnp.asarray(sizes, jnp.int32))

    sizes = jnp.where(number % 4 == 0, named(crowded, number // 4), named(usual, number - number // 4 - 1))
    mixed = jax.random.permutation(jax.random.fold_in(own, 3), number_of)
    giver, receiver = mixed[0:number_of // 2 * 2:2], mixed[1:number_of // 2 * 2:2]
    margin = jnp.minimum(sizes[giver] - 1, most - sizes[receiver]) // 2
    margin = jnp.where((giver == sequence[0]) | (receiver == sequence[0]) | (sizes[receiver] == 0), 0, jnp.maximum(margin, 0))
    passed = jax.random.randint(jax.random.fold_in(own, 4), (number_of // 2,), 0, 1 << 20) % (margin + 1)
    sizes = sizes.at[giver].add(-passed).at[receiver].add(passed)
    labels = jnp.searchsorted(jnp.cumsum(sizes), jnp.arange(rows * top), side="right").astype(jnp.int32)
    table = labels.reshape(top, rows).T
    table = table[jax.random.permutation(jax.random.fold_in(own, 1), rows)]
    offset_by = jax.random.randint(jax.random.fold_in(own, 2), (rows, 1), 0, top)
    return jnp.take_along_axis(table, (jnp.arange(top)[None, :] + offset_by) % top, axis=1)


def load_shares(amount, total, bound, skew, full):
    portions = [(1 << 20) // math.isqrt(rank ** skew) + 1 for rank in range(1, amount + 1)]
    largest = bound if full else min(bound, max(-(-total // amount), total * portions[0] // sum(portions)))
    least = 1 if total - largest >= amount - 1 else 0
    counts, spare = [largest] + [least] * (amount - 1), total - largest - least * (amount - 1)
    while spare > 0:
        candidates = [i for i in range(1, amount) if counts[i] < largest] or [i for i in range(1, amount) if counts[i] < bound]
        whole, left = sum([portions[i] for i in candidates]), spare
        for i in candidates:
            addition = min(bound - counts[i], max(1, left * portions[i] // whole), spare)
            counts[i] = counts[i] + addition
            spare = spare - addition
    return np.array(counts)


def centred(stream_key, extent, deviation, most, cuts=(), kind=jnp.bfloat16):
    factor_of = level_of(stream_key, extent, cuts, -0.22, 0.18) if cuts else 1.0
    result = jax.random.normal(stream_key, extent, jnp.float32) * deviation * factor_of
    return jnp.minimum(jnp.maximum(result, -most), most).astype(kind)


def setup_inputs(seed: int = 0, part: int = 0) -> dict:
    key_list = jax.random.split(jax.random.key(seed), 12)
    own_keys = jax.random.split(jax.random.fold_in(key_list[11], part), 12)
    stream = draw_stream(jax.random.fold_in(jax.random.fold_in(key_list[11], part), 71), part)
    query_proj = draw_query_proj(jax.random.fold_in(jax.random.fold_in(key_list[11], part), 71), part)
    key_proj = draw_key_proj(jax.random.fold_in(jax.random.fold_in(key_list[11], part), 71), part)
    value_projected = centred(own_keys[3], (BLOCK_TOKENS, KEY_VALUE_HEADS * HEAD_SIZE), 1.0, 6.0, ((0, 4),))
    expert_ids_keys = jax.random.split(jax.random.fold_in(own_keys[4], 1), BLOCK_TOKENS // TOK_DEV)
    expert_ids_turns = jax.random.permutation(jax.random.fold_in(own_keys[4], 3), BLOCK_TOKENS // TOK_DEV)
    expert_ids = jax.vmap(lambda own, number: deal_out(jax.random.fold_in(own_keys[4], 2), own, number, TOK_DEV, EXPERTS, TOP, CAP, 2))(expert_ids_keys, expert_ids_turns).reshape((BLOCK_TOKENS, TOP))
    expert_home = jax.random.permutation(key_list[5], EXPERTS).astype(jnp.int32)
    router = centred(key_list[6], (D, EXPERTS), D ** -0.5, 0.09375, ((0, 4),))
    norm_gain = jnp.clip(1.0 + 0.15 * jax.random.normal(key_list[7], (D,), jnp.float32), 0.25, 1.75).astype(jnp.bfloat16)
    w_gate = centred(key_list[8], (EXPERTS, D, HID), D ** -0.5, 0.09375, ((0, 4), (1, 4)))
    w_up = centred(key_list[9], (EXPERTS, D, HID), D ** -0.5, 0.09375, ((0, 4), (1, 4)))
    w_down = centred(key_list[10], (EXPERTS, HID, D), HID ** -0.5, 0.21875, ((0, 4), (2, 4)))
    return dict(stream=stream, query_proj=query_proj, key_proj=key_proj, value_projected=value_projected, expert_ids=expert_ids, expert_home=expert_home, router=router, norm_gain=norm_gain, w_gate=w_gate, w_up=w_up, w_down=w_down)


epsilon = 1e-06

def attention_rows(query_block_rows, first_row, key_gathered, value_gathered):
    block_length_rows = query_block_rows.shape[0]
    query_matrix = query_block_rows.astype(jnp.float32).reshape(block_length_rows, KEY_VALUE_HEADS, QUERY_HEADS // KEY_VALUE_HEADS, HEAD_SIZE)
    key_subset = key_gathered.astype(jnp.float32).reshape(BLOCK_TOKENS, KEY_VALUE_HEADS, HEAD_SIZE)
    value_subset = value_gathered.astype(jnp.float32).reshape(BLOCK_TOKENS, KEY_VALUE_HEADS, HEAD_SIZE)
    scores = jnp.einsum('tgha,pga->ghtp', query_matrix, key_subset) * (1.0 / math.sqrt(HEAD_SIZE))
    query_pos = first_row + jnp.arange(block_length_rows, dtype=jnp.int32)
    key_pos = jnp.arange(BLOCK_TOKENS, dtype=jnp.int32)
    visible = query_pos[:, None] >= key_pos[None, :]
    scores = jnp.where(visible, scores, -1e+30)
    top_score = lax.optimization_barrier(jnp.max(scores, axis=-1, keepdims=True))
    expo = jnp.where(visible, jnp.exp(scores - top_score), 0.0)
    total = lax.optimization_barrier(jnp.sum(expo, axis=-1))
    rounded = lax.optimization_barrier(expo.astype(jnp.bfloat16))
    mixed = jnp.einsum('ghtp,pga->ghta', rounded.astype(jnp.float32), value_subset) / total[..., None]
    return jnp.transpose(mixed, (2, 0, 1, 3)).reshape(block_length_rows, QUERY_HEADS * HEAD_SIZE)

def block_attention(queries, key_gathered, value_gathered):
    blocks = BLOCK_TOKENS // TOK_DEV
    query_blocks = queries.reshape(blocks, TOK_DEV, QUERY_HEADS * HEAD_SIZE)
    firsts = jnp.arange(blocks, dtype=jnp.int32) * TOK_DEV

    def one_block(packed):
        return attention_rows(packed[0], packed[1], key_gathered, value_gathered)
    return lax.map(one_block, (query_blocks, firsts)).reshape(BLOCK_TOKENS, QUERY_HEADS * HEAD_SIZE)

def split_product(row_block, weight):
    shards = N_SECTION * N_REP
    width = D // shards
    rows = row_block.astype(jnp.float32).reshape(row_block.shape[0], shards, width)
    parts = weight.astype(jnp.float32).reshape(shards, width, HID)
    partial_value = jnp.einsum('rsd,sdh->srh', rows, parts)
    rounded = lax.optimization_barrier(partial_value.astype(jnp.bfloat16))
    return lax.optimization_barrier(jnp.sum(rounded.astype(jnp.float32), axis=0))

def expert_mix(normed, chosen, gates, home_row, gate_set, up_set, down_set):
    flat_ids = chosen.reshape(-1).astype(jnp.int32)
    flat_tok = (jnp.arange(BLOCK_TOKENS * TOP, dtype=jnp.int32) // TOP).astype(jnp.int32)
    flat_gate = gates.reshape(-1)
    limit = EXPERTS * CAP

    def visit(total, expert):
        member = flat_ids == expert
        row_index = jnp.nonzero(member, size=limit, fill_value=0)[0].astype(jnp.int32)
        live = (jnp.arange(limit, dtype=jnp.int32) < jnp.sum(member.astype(jnp.int32))).astype(jnp.float32)
        token_index = flat_tok[row_index]
        row_block = normed[token_index]
        device_slot = home_row[expert]
        gate_act = split_product(row_block, gate_set[device_slot])
        up_act = split_product(row_block, up_set[device_slot])
        product = (jax.nn.silu(gate_act) * up_act).astype(jnp.bfloat16)
        answer = jnp.dot(product, down_set[device_slot], preferred_element_type=jnp.float32).astype(jnp.bfloat16)
        answer = lax.optimization_barrier(answer)
        weight_col = flat_gate[row_index] * live
        total = total.at[token_index].add(weight_col[:, None] * answer.astype(jnp.float32))
        return (total, None)
    total, ignored = lax.scan(visit, jnp.zeros((BLOCK_TOKENS, D), jnp.float32), jnp.arange(EXPERTS, dtype=jnp.int32))
    return total

def reference(stream, query_proj, key_proj, value_projected, expert_ids, expert_home, router, norm_gain, w_gate, w_up, w_down):
    attended = block_attention(query_proj, key_proj, value_projected)
    hidden = stream.astype(jnp.float32) + attended
    mean_sq = lax.optimization_barrier(jnp.mean(hidden * hidden, axis=-1, keepdims=True))
    normed = (hidden * lax.rsqrt(mean_sq + epsilon) * norm_gain.astype(jnp.float32)).astype(jnp.bfloat16)
    logits = jnp.dot(normed, router, preferred_element_type=jnp.float32)
    picked = jnp.take_along_axis(logits, expert_ids.astype(jnp.int32), axis=1)
    squashed = jax.nn.sigmoid(picked)
    gates = squashed / lax.optimization_barrier(jnp.sum(squashed, axis=-1, keepdims=True))
    mixed = expert_mix(normed, expert_ids, gates, expert_home.astype(jnp.int32), w_gate, w_up, w_down)
    return (hidden + mixed).astype(jnp.bfloat16)
```

```python
import functools
import math

import jax
import jax.numpy as jnp
from jax import lax
from jax.experimental import pallas as pl
from jax.experimental.pallas import tpu as pltpu
from jax.sharding import PartitionSpec as P

HEAD_SIZE = 128
epsilon = 1e-06
very_negative = -1e30
MESH = pl.DeviceIdType.MESH
F32 = jnp.float32
BF16 = jnp.bfloat16


def dot(a, b):
    return jnp.dot(a, b, preferred_element_type=F32)


def body(
    C, S, R, cap,
    stream_ref, q_ref, k_ref, v_ref, ids_ref, home_ref, router_ref, gain_ref,
    wg_hbm, wu_hbm, wd_hbm,
    out_ref,
    wg, wu, wd, qs, kbuf, vbuf, sbuf, mbuf, lbuf, acc, hid, nrm, ssbuf, lgbuf,
    place, dsrc, dbuf, asrc, abuf, bsrc, bbuf, ibuf, ysrc, ybuf,
    w_sem, k_send, k_recv, v_send, v_recv, ss_send, ss_recv, lg_send, lg_recv,
    d_send, d_recv, a_send, a_recv, b_send, b_recv, i_send, i_recv, y_send, y_recv,
):
    T, W = stream_ref.shape
    H = W // HEAD_SIZE
    F = S * R
    E = router_ref.shape[1]
    HID = wg.shape[1]
    HR = HID // R
    top = ids_ref.shape[1]
    me = lax.axis_index("ctx")
    sec = lax.axis_index("section")
    rep = lax.axis_index("rep")
    f = sec * R + rep
    kv_heads = k_ref.shape[1] // HEAD_SIZE
    kv = f * H // (H * F // kv_heads)

    def ctx_dev(d):
        return {"ctx": lax.rem(me + d + C, C)}

    def feat(j):
        return lax.rem(f + j, F)

    def feat_dev(j):
        g = feat(j)
        return {"section": g // R, "rep": lax.rem(g, R)}

    def rc(src, dst, ss, rs, dev):
        return pltpu.make_async_remote_copy(
            src_ref=src, dst_ref=dst, send_sem=ss, recv_sem=rs,
            device_id=dev, device_id_type=MESH,
        )

    weights = [
        pltpu.make_async_copy(wg_hbm.at[0], wg, w_sem.at[0]),
        pltpu.make_async_copy(wu_hbm.at[0], wu, w_sem.at[1]),
        pltpu.make_async_copy(wd_hbm.at[0], wd, w_sem.at[2]),
    ]
    for c in weights:
        c.start()

    barrier = pltpu.get_barrier_semaphore()
    for d in range(1, C):
        pl.semaphore_signal(barrier, inc=1, device_id=ctx_dev(d), device_id_type=MESH)
    for j in range(1, F):
        pl.semaphore_signal(barrier, inc=1, device_id=feat_dev(j), device_id_type=MESH)
    pl.semaphore_wait(barrier, C - 1 + F - 1)

    kcols = pl.ds(pl.multiple_of(kv * HEAD_SIZE, HEAD_SIZE), HEAD_SIZE)

    def kcopy(d):
        return rc(k_ref.at[:, kcols], kbuf.at[d], k_send.at[d], k_recv.at[d], ctx_dev(d))

    def vcopy(d):
        return rc(v_ref.at[:, kcols], vbuf.at[d], v_send.at[d], v_recv.at[d], ctx_dev(d))

    @pl.loop(1, C - me)
    def _(d):
        kcopy(d).start()

    @pl.loop(1, C - me)
    def _(d):
        vcopy(d).start()

    kbuf[0] = k_ref[:, kcols]
    vbuf[0] = v_ref[:, kcols]
    for h in range(H):
        qs[h * T : (h + 1) * T, :] = q_ref[:, h * HEAD_SIZE : (h + 1) * HEAD_SIZE]
    scale = 1.0 / math.sqrt(HEAD_SIZE)

    def scores(d):
        return (
            lax.dot_general(
                qs[...], kbuf[d], (((1,), (1,)), ((), ())), preferred_element_type=F32
            )
            * scale
        )

    row_t = lax.broadcasted_iota(jnp.int32, (T, T), 0)
    col_t = lax.broadcasted_iota(jnp.int32, (T, T), 1)
    s0 = scores(0)
    seen = jnp.concatenate([row_t >= col_t] * H, axis=0)
    s0 = jnp.where(seen, s0, very_negative)
    sbuf[0] = s0
    mbuf[...] = s0

    ids = ids_ref[...]
    dest = jnp.zeros_like(ids)
    for e in range(E):
        dest = jnp.where(ids == e, home_ref[e], dest)
    rel = dest - me
    rel = jnp.where(rel < 0, rel + C, rel)
    lanes = lax.broadcasted_iota(jnp.int32, (T, 128), 1)
    hot = jnp.zeros((T, 128), F32)
    for k in range(top):
        hot = hot + jnp.where(rel[:, k : k + 1] == lanes, 1.0, 0.0)
    lower = jnp.where(row_t > col_t, 1.0, 0.0).astype(BF16)
    rank = dot(lower, hot.astype(BF16))
    slots = lax.broadcasted_iota(jnp.int32, (T, cap), 1).astype(F32)
    for d in range(C):
        chosen = (hot[:, d : d + 1] > 0.5) & (rank[:, d : d + 1] == slots)
        place[d] = jnp.where(chosen, 1.0, 0.0).astype(BF16)

    @pl.loop(1, me + 1)
    def _(d):
        kcopy(d).wait_recv()
        s = scores(d)
        sbuf[d] = s
        mbuf[...] = jnp.maximum(mbuf[...], s)

    row_max = jnp.max(mbuf[...], axis=-1, keepdims=True)
    mbuf[...] = jnp.broadcast_to(row_max, mbuf.shape)
    e0 = jnp.exp(sbuf[0] - mbuf[...])
    lbuf[...] = e0
    acc[...] = dot(e0.astype(BF16), vbuf[0])

    @pl.loop(1, me + 1)
    def _(d):
        vcopy(d).wait_recv()
        ex = jnp.exp(sbuf[d] - mbuf[...])
        lbuf[...] = lbuf[...] + ex
        acc[...] = acc[...] + dot(ex.astype(BF16), vbuf[d])

    sq = jnp.zeros((T, HEAD_SIZE), F32)
    for h in range(H):
        rows = slice(h * T, (h + 1) * T)
        cols = slice(h * HEAD_SIZE, (h + 1) * HEAD_SIZE)
        total = jnp.sum(lbuf[rows, :], axis=-1, keepdims=True)
        hv = stream_ref[:, cols].astype(F32) + acc[rows, :] / total
        hid[:, cols] = hv
        sq = sq + hv * hv
    eye = row_t == col_t

    def to_row(col):
        return jnp.sum(jnp.where(eye, col, 0.0), axis=0, keepdims=True)

    def to_col(row):
        return jnp.sum(jnp.where(eye, row, 0.0), axis=1, keepdims=True)

    ssbuf[f] = jnp.broadcast_to(to_row(jnp.sum(sq, axis=-1, keepdims=True)), (8, T))

    def sscopy(j, owner):
        return rc(ssbuf.at[owner], ssbuf.at[owner], ss_send.at[j], ss_recv.at[owner], feat_dev(j))

    def lgcopy(j, owner):
        return rc(lgbuf.at[owner], lgbuf.at[owner], lg_send.at[j], lg_recv.at[owner], feat_dev(j))

    for j in range(1, F):
        sscopy(j, f).start()
    for j in range(1, F):
        sscopy(j, feat(j)).wait_recv()
    ss = ssbuf[0]
    for g in range(1, F):
        ss = ss + ssbuf[g]
    scale_rows = lax.rsqrt(to_col(ss[0:1, :]) / (W * F) + epsilon)
    nrm[...] = (hid[...] * scale_rows * gain_ref[...].astype(F32)).astype(BF16)

    def dcopy(d):
        return rc(dsrc.at[d], dbuf.at[d], d_send.at[d], d_recv.at[d], ctx_dev(d))

    def gathered(d):
        return lax.dot_general(
            place[d], nrm[...], (((0,), (0,)), ((), ())), preferred_element_type=F32
        ).astype(BF16)

    @pl.loop(1, C)
    def _(d):
        dsrc[d] = gathered(d)
        dcopy(d).start()

    dbuf[0] = gathered(0)

    lg = dot(nrm[...], router_ref[...])
    for e in range(E):
        lgbuf[f, e : e + 1, :] = to_row(lg[:, e : e + 1])
    for j in range(1, F):
        lgcopy(j, f).start()

    for c in weights:
        c.wait()

    def rep_at(j):
        return lax.rem(rep + j, R)

    def sec_at(j):
        return lax.rem(sec + j, S)

    def acopy(d, j, owner):
        return rc(
            asrc.at[d, rep_at(j)], abuf.at[d, owner], a_send.at[d, j], a_recv.at[d, owner],
            {"rep": rep_at(j)},
        )

    def bcopy(d, j, owner):
        return rc(
            bsrc.at[d], bbuf.at[d, owner], b_send.at[d, j], b_recv.at[d, owner],
            {"section": sec_at(j)},
        )

    def icopy(d, j, owner):
        return rc(
            ibuf.at[d, owner], ibuf.at[d, owner], i_send.at[d, j], i_recv.at[d, owner],
            {"rep": rep_at(j)},
        )

    def ycopy(d):
        return rc(ysrc.at[d], ybuf.at[d], y_send.at[d], y_recv.at[d], ctx_dev(-d))

    def stage_g(d):
        x = dbuf[d]
        for r in range(R):
            cols = slice(r * HR, (r + 1) * HR)
            asrc[d, r, :, 0:HR] = dot(x, wg[:, cols]).astype(BF16)
            asrc[d, r, :, HR : 2 * HR] = dot(x, wu[:, cols]).astype(BF16)
        for j in range(1, R):
            acopy(d, j, rep).start()

    def stage_b(d):
        total = asrc[d, rep].astype(F32)
        for j in range(1, R):
            acopy(d, j, rep_at(j)).wait_recv()
            total = total + abuf[d, rep_at(j)].astype(F32)
        bsrc[d] = total.astype(BF16)
        for j in range(1, S):
            bcopy(d, j, sec).start()

    def stage_i(d):
        total = bsrc[d].astype(F32)
        for j in range(1, S):
            bcopy(d, j, sec_at(j)).wait_recv()
            total = total + bbuf[d, sec_at(j)].astype(F32)
        g = total[:, 0:HR]
        u = total[:, HR : 2 * HR]
        ibuf[d, rep] = (g * jax.nn.sigmoid(g) * u).astype(BF16)
        for j in range(1, R):
            icopy(d, j, rep).start()

    def stage_d(d):
        for j in range(1, R):
            icopy(d, j, rep_at(j)).wait_recv()
        y = dot(ibuf[d, 0], wd[0:HR, :])
        for r in range(1, R):
            y = y + dot(ibuf[d, r], wd[r * HR : (r + 1) * HR, :])
        return y.astype(BF16)

    stage_g(0)
    stage_b(0)

    def finish(d):
        stage_i(d)
        y = stage_d(d)
        return y

    if C > 1:
        dcopy(1).wait_recv()
        stage_g(1)
        stage_b(1)
    ybuf[0] = finish(0)

    @pl.loop(2, C)
    def _(d):
        dcopy(d).wait_recv()
        stage_g(d)
        stage_b(d)
        ysrc[d - 1] = finish(d - 1)
        ycopy(d - 1).start()

    if C > 1:
        ysrc[C - 1] = finish(C - 1)
        ycopy(C - 1).start()

    for j in range(1, F):
        lgcopy(j, feat(j)).wait_recv()
    lt = lgbuf[0]
    for g in range(1, F):
        lt = lt + lgbuf[g]
    picked = jnp.zeros(ids.shape, F32)
    for e in range(E):
        picked = jnp.where(ids == e, to_col(lt[e : e + 1, :]), picked)
    squashed = jax.nn.sigmoid(picked)
    gates = squashed / jnp.sum(squashed, axis=-1, keepdims=True)

    def weighted(d):
        gd = jnp.sum(jnp.where(rel == d, gates, 0.0), axis=-1, keepdims=True)
        return gd * dot(place[d], ybuf[d])

    hid[...] = hid[...] + weighted(0)

    @pl.loop(1, C)
    def _(d):
        ycopy(d).wait_recv()
        hid[...] = hid[...] + weighted(d)

    out_ref[...] = hid[...].astype(BF16)

    @pl.loop(1, C - me)
    def _(d):
        kcopy(d).wait_send()
        vcopy(d).wait_send()

    for j in range(1, F):
        sscopy(j, f).wait_send()
        lgcopy(j, f).wait_send()

    @pl.loop(0, C)
    def _(d):
        for j in range(1, R):
            acopy(d, j, rep).wait_send()
            icopy(d, j, rep).wait_send()
        for j in range(1, S):
            bcopy(d, j, sec).wait_send()

    @pl.loop(1, C)
    def _(d):
        dcopy(d).wait_send()
        ycopy(d).wait_send()


def local(C, S, R, stream, q, k, v, ids, home, router, gain, w_gate, w_up, w_down):
    T, W = stream.shape
    top = ids.shape[1]
    H = W // HEAD_SIZE
    F = S * R
    E = router.shape[1]
    HID = w_gate.shape[2]
    HR = HID // R
    capacity = min(T, max(2, 5 * T * top // (4 * C)))
    cap = -(-capacity // 16) * 16
    e_rows = -(-E // 8) * 8
    DMA = pltpu.SemaphoreType.DMA
    vmem = pl.BlockSpec(memory_space=pltpu.VMEM)
    smem = pl.BlockSpec(memory_space=pltpu.SMEM)
    hbm = pl.BlockSpec(memory_space=pl.ANY)
    V = pltpu.VMEM
    return pl.pallas_call(
        functools.partial(body, C, S, R, cap),
        out_shape=jax.ShapeDtypeStruct((T, W), BF16),
        in_specs=[vmem] * 5 + [smem] + [vmem] * 2 + [hbm] * 3,
        out_specs=vmem,
        scratch_shapes=[
            V((W, HID), BF16), V((W, HID), BF16), V((HID, W), BF16),
            V((H * T, HEAD_SIZE), BF16),
            V((C, T, HEAD_SIZE), BF16), V((C, T, HEAD_SIZE), BF16),
            V((C, H * T, T), F32), V((H * T, T), F32), V((H * T, T), F32),
            V((H * T, HEAD_SIZE), F32),
            V((T, W), F32), V((T, W), BF16),
            V((F, 8, T), F32), V((F, e_rows, T), F32),
            V((C, T, cap), BF16),
            V((C, cap, W), BF16), V((C, cap, W), BF16),
            V((C, R, cap, 2 * HR), BF16), V((C, R, cap, 2 * HR), BF16),
            V((C, cap, 2 * HR), BF16), V((C, S, cap, 2 * HR), BF16),
            V((C, R, cap, HR), BF16),
            V((C, cap, W), BF16), V((C, cap, W), BF16),
            DMA((3,)),
            DMA((C,)), DMA((C,)), DMA((C,)), DMA((C,)),
            DMA((F,)), DMA((F,)), DMA((F,)), DMA((F,)),
            DMA((C,)), DMA((C,)),
            DMA((C, R)), DMA((C, R)),
            DMA((C, S)), DMA((C, S)),
            DMA((C, R)), DMA((C, R)),
            DMA((C,)), DMA((C,)),
        ],
        compiler_params=pltpu.CompilerParams(
            collective_id=0, has_side_effects=True, vmem_limit_bytes=62 * 1024 * 1024
        ),
        name="block",
    )(stream, q, k, v, ids, home, router, gain.reshape(1, W), w_gate, w_up, w_down)


def solution(mesh):
    placed = (
        P(("group", "ctx"), ("section", "rep")),
        P(("group", "ctx"), ("section", "rep")),
        P(("group", "ctx"), None),
        P(("group", "ctx"), None),
        P(("group", "ctx"), None),
        P(),
        P(("section", "rep"), None),
        P(("section", "rep")),
        P("ctx", ("section", "rep"), None),
        P("ctx", ("section", "rep"), None),
        P("ctx", None, ("section", "rep")),
    )
    return jax.shard_map(
        functools.partial(
            local, mesh.shape["ctx"], mesh.shape["section"], mesh.shape["rep"]
        ),
        mesh=mesh,
        in_specs=placed,
        out_specs=P(("group", "ctx"), ("section", "rep")),
        check_vma=False,
    )
```

```python
import functools
import math

import jax
import jax.numpy as jnp
from jax import lax
from jax.experimental import pallas as pl
from jax.experimental.pallas import tpu as pltpu
from jax.sharding import PartitionSpec as P

HEAD_SIZE = 128
epsilon = 1e-06
very_negative = -1e30
MESH = pl.DeviceIdType.MESH
F32 = jnp.float32
BF16 = jnp.bfloat16


def dot(a, b):
    return jnp.dot(a, b, preferred_element_type=F32)


def body(
    C, S, R, cap,
    stream_hbm, q_hbm, k_hbm, v_hbm, ids_hbm, home_ref, router_hbm, gain_hbm,
    wg_hbm, wu_hbm, wd_hbm,
    out_ref,
    stream_ref, q_ref, k_ref, v_ref, ids_ref, router_ref, gain_ref,
    wg, wu, wd, qs, kbuf, vbuf, sbuf, mbuf, lbuf, acc, hid, nrm, ssbuf, lgbuf,
    place, scsrc, scbuf, dsrc, dbuf, asrc, abuf, bsrc, bbuf, ibuf, ysrc, ybuf,
    w_sem, x_sem, c_send, c_recv, k_send, k_recv, v_send, v_recv, ss_send, ss_recv, lg_send, lg_recv,
    d_send, d_recv, a_send, a_recv, b_send, b_recv, i_send, i_recv, y_send, y_recv,
):
    T, W = stream_ref.shape
    H = W // HEAD_SIZE
    F = S * R
    E = router_ref.shape[0]
    HID = wg.shape[1]
    HR = HID // R
    top = ids_ref.shape[0]
    me = lax.axis_index("ctx")
    sec = lax.axis_index("section")
    rep = lax.axis_index("rep")
    f = sec * R + rep
    kv_heads = k_ref.shape[1] // HEAD_SIZE
    kv = f * H // (H * F // kv_heads)

    def ctx_dev(d):
        return {"ctx": lax.rem(me + d + C, C)}

    def feat(j):
        return lax.rem(f + j, F)

    def feat_dev(j):
        g = feat(j)
        return {"section": g // R, "rep": lax.rem(g, R)}

    def rc(src, dst, ss, rs, dev):
        return pltpu.make_async_remote_copy(
            src_ref=src, dst_ref=dst, send_sem=ss, recv_sem=rs,
            device_id=dev, device_id_type=MESH,
        )

    weights = [
        pltpu.make_async_copy(wg_hbm.at[0], wg, w_sem.at[0]),
        pltpu.make_async_copy(wu_hbm.at[0], wu, w_sem.at[1]),
        pltpu.make_async_copy(wd_hbm.at[0], wd, w_sem.at[2]),
    ]
    staged = [
        pltpu.make_async_copy(src, dst, x_sem.at[i])
        for i, (src, dst) in enumerate(
            (
                (k_hbm, k_ref), (v_hbm, v_ref), (q_hbm, q_ref), (ids_hbm, ids_ref),
                (stream_hbm, stream_ref), (gain_hbm, gain_ref), (router_hbm, router_ref),
            )
        )
    ]
    for c in staged:
        c.start()
    for c in weights:
        c.start()

    barrier = pltpu.get_barrier_semaphore()
    for d in range(1, C):
        pl.semaphore_signal(barrier, inc=1, device_id=ctx_dev(d), device_id_type=MESH)
    for j in range(1, F):
        pl.semaphore_signal(barrier, inc=1, device_id=feat_dev(j), device_id_type=MESH)
    staged[0].wait()
    staged[1].wait()
    pl.semaphore_wait(barrier, C - 1 + F - 1)

    kcols = pl.ds(pl.multiple_of(kv * HEAD_SIZE, HEAD_SIZE), HEAD_SIZE)

    def kcopy(d):
        return rc(k_ref.at[:, kcols], kbuf.at[d], k_send.at[d], k_recv.at[d], ctx_dev(d))

    def vcopy(d):
        return rc(v_ref.at[:, kcols], vbuf.at[d], v_send.at[d], v_recv.at[d], ctx_dev(d))

    @pl.loop(1, C - me)
    def _(d):
        kcopy(d).start()

    @pl.loop(1, C - me)
    def _(d):
        vcopy(d).start()

    for c in staged[2:]:
        c.wait()
    kbuf[0] = k_ref[:, kcols]
    vbuf[0] = v_ref[:, kcols]
    for h in range(H):
        qs[h * T : (h + 1) * T, :] = q_ref[:, h * HEAD_SIZE : (h + 1) * HEAD_SIZE]
    scale = 1.0 / math.sqrt(HEAD_SIZE)

    def scores(d):
        return (
            lax.dot_general(
                qs[...], kbuf[d], (((1,), (1,)), ((), ())), preferred_element_type=F32
            )
            * scale
        )

    row_t = lax.broadcasted_iota(jnp.int32, (T, T), 0)
    col_t = lax.broadcasted_iota(jnp.int32, (T, T), 1)
    s0 = scores(0)
    seen = jnp.concatenate([row_t >= col_t] * H, axis=0)
    s0 = jnp.where(seen, s0, very_negative)
    sbuf[0] = s0
    mbuf[...] = s0

    eye = row_t == col_t

    def to_row(col):
        return jnp.sum(jnp.where(eye, col, 0.0), axis=0, keepdims=True)

    def to_col(row):
        return jnp.sum(jnp.where(eye, row, 0.0), axis=1, keepdims=True)

    ids = ids_ref[...]
    dest = jnp.zeros_like(ids)
    for e in range(E):
        dest = jnp.where(ids == e, home_ref[e], dest)
    rel = dest - me
    rel = jnp.where(rel < 0, rel + C, rel)
    lanes = lax.broadcasted_iota(jnp.int32, (T, 128), 1)
    hot = jnp.zeros((T, 128), F32)
    rel_cols = [to_col(rel[k : k + 1, :].astype(F32)).astype(jnp.int32) for k in range(top)]
    for k in range(top):
        hot = hot + jnp.where(rel_cols[k] == lanes, 1.0, 0.0)
    lower = jnp.where(row_t > col_t, 1.0, 0.0).astype(BF16)
    rank = dot(lower, hot.astype(BF16))
    slots = lax.broadcasted_iota(jnp.int32, (T, cap), 1).astype(F32)
    for d in range(C):
        chosen = (hot[:, d : d + 1] > 0.5) & (rank[:, d : d + 1] == slots)
        place[d] = jnp.where(chosen, 1.0, 0.0).astype(BF16)

    @pl.loop(1, me + 1)
    def _(d):
        kcopy(d).wait_recv()
        s = scores(d)
        sbuf[d] = s
        mbuf[...] = jnp.maximum(mbuf[...], s)

    row_max = jnp.max(mbuf[...], axis=-1, keepdims=True)
    mbuf[...] = jnp.broadcast_to(row_max, mbuf.shape)
    e0 = jnp.exp(sbuf[0] - mbuf[...])
    lbuf[...] = e0
    acc[...] = dot(e0.astype(BF16), vbuf[0])

    @pl.loop(1, me + 1)
    def _(d):
        vcopy(d).wait_recv()
        ex = jnp.exp(sbuf[d] - mbuf[...])
        lbuf[...] = lbuf[...] + ex
        acc[...] = acc[...] + dot(ex.astype(BF16), vbuf[d])

    sq = jnp.zeros((T, HEAD_SIZE), F32)
    for h in range(H):
        rows = slice(h * T, (h + 1) * T)
        cols = slice(h * HEAD_SIZE, (h + 1) * HEAD_SIZE)
        total = jnp.sum(lbuf[rows, :], axis=-1, keepdims=True)
        hv = stream_ref[:, cols].astype(F32) + acc[rows, :] / total
        hid[:, cols] = hv
        sq = sq + hv * hv
    ssbuf[f] = jnp.broadcast_to(to_row(jnp.sum(sq, axis=-1, keepdims=True)), (8, T))

    def sscopy(j, owner):
        return rc(ssbuf.at[owner], ssbuf.at[owner], ss_send.at[j], ss_recv.at[owner], feat_dev(j))

    def lgcopy(j, owner):
        return rc(lgbuf.at[owner], lgbuf.at[owner], lg_send.at[j], lg_recv.at[owner], feat_dev(j))

    for j in range(1, F):
        sscopy(j, f).start()
    gain = gain_ref[...].astype(F32).reshape(1, W)
    nrm[...] = (hid[...] * gain).astype(BF16)

    def dcopy(d):
        return rc(dsrc.at[d], dbuf.at[d], d_send.at[d], d_recv.at[d], ctx_dev(d))

    def gathered(d):
        return lax.dot_general(
            place[d], nrm[...], (((0,), (0,)), ((), ())), preferred_element_type=F32
        ).astype(BF16)

    @pl.loop(1, C)
    def _(d):
        dsrc[d] = gathered(d)
        dcopy(d).start()

    dbuf[0] = gathered(0)

    for c in weights:
        c.wait()

    def rep_at(j):
        return lax.rem(rep + j, R)

    def sec_at(j):
        return lax.rem(sec + j, S)

    def acopy(d, j, owner):
        return rc(
            asrc.at[d, rep_at(j)], abuf.at[d, owner], a_send.at[d, j], a_recv.at[d, owner],
            {"rep": rep_at(j)},
        )

    def bcopy(d, j, owner):
        return rc(
            bsrc.at[d], bbuf.at[d, owner], b_send.at[d, j], b_recv.at[d, owner],
            {"section": sec_at(j)},
        )

    def icopy(d, j, owner):
        return rc(
            ibuf.at[d, owner], ibuf.at[d, owner], i_send.at[d, j], i_recv.at[d, owner],
            {"rep": rep_at(j)},
        )

    def ycopy(d):
        return rc(ysrc.at[d], ybuf.at[d], y_send.at[d], y_recv.at[d], ctx_dev(-d))

    def stage_g(d):
        x = dbuf[d]
        for r in range(R):
            cols = slice(r * HR, (r + 1) * HR)
            asrc[d, r, :, 0:HR] = dot(x, wg[:, cols]).astype(BF16)
            asrc[d, r, :, HR : 2 * HR] = dot(x, wu[:, cols]).astype(BF16)
        for j in range(1, R):
            acopy(d, j, rep).start()

    def stage_b(d):
        total = asrc[d, rep].astype(F32)
        for j in range(1, R):
            acopy(d, j, rep_at(j)).wait_recv()
            total = total + abuf[d, rep_at(j)].astype(F32)
        bsrc[d] = total.astype(BF16)
        for j in range(1, S):
            bcopy(d, j, sec).start()

    eye_cap = lax.broadcasted_iota(jnp.int32, (cap, cap), 0) == lax.broadcasted_iota(
        jnp.int32, (cap, cap), 1
    )

    def ccopy(d):
        return rc(scsrc.at[d], scbuf.at[d], c_send.at[d], c_recv.at[d], ctx_dev(d))

    def rows_scale(d):
        return jnp.sum(jnp.where(eye_cap, scbuf[d, 0:1, 0:cap], 0.0), axis=1, keepdims=True)

    def stage_i(d):
        total = bsrc[d].astype(F32)
        for j in range(1, S):
            bcopy(d, j, sec_at(j)).wait_recv()
            total = total + bbuf[d, sec_at(j)].astype(F32)
        total = total * rows_scale(d)
        g = total[:, 0:HR]
        u = total[:, HR : 2 * HR]
        ibuf[d, rep] = (g * jax.nn.sigmoid(g) * u).astype(BF16)
        for j in range(1, R):
            icopy(d, j, rep).start()

    def stage_d(d):
        for j in range(1, R):
            icopy(d, j, rep_at(j)).wait_recv()
        y = dot(ibuf[d, 0], wd[0:HR, :])
        for r in range(1, R):
            y = y + dot(ibuf[d, r], wd[r * HR : (r + 1) * HR, :])
        return y.astype(BF16)

    stage_g(0)

    for j in range(1, F):
        sscopy(j, feat(j)).wait_recv()
    ss = ssbuf[0]
    for g in range(1, F):
        ss = ss + ssbuf[g]
    scale_rows = lax.rsqrt(to_col(ss[0:1, :]) / (W * F) + epsilon)

    def slot_scale(d):
        return jnp.sum(jnp.where(place[d].astype(F32) > 0.5, scale_rows, 0.0), axis=0, keepdims=True)

    @pl.loop(1, C)
    def _(d):
        scsrc[d, 0:1, 0:cap] = slot_scale(d)
        ccopy(d).start()

    scbuf[0, 0:1, 0:cap] = slot_scale(0)

    stage_b(0)

    normed = (hid[...] * scale_rows * gain).astype(BF16)
    lgbuf[f, 0:E, :] = lax.dot_general(
        router_ref[...], normed, (((1,), (1,)), ((), ())), preferred_element_type=F32
    )
    for j in range(1, F):
        lgcopy(j, f).start()

    def finish(d):
        stage_i(d)
        y = stage_d(d)
        return y

    if C > 1:
        dcopy(1).wait_recv()
        stage_g(1)
        stage_b(1)
    ybuf[0] = finish(0)

    @pl.loop(2, C)
    def _(d):
        dcopy(d).wait_recv()
        stage_g(d)
        stage_b(d)
        ccopy(d - 1).wait_recv()
        ysrc[d - 1] = finish(d - 1)
        ycopy(d - 1).start()

    if C > 1:
        ccopy(C - 1).wait_recv()
        ysrc[C - 1] = finish(C - 1)
        ycopy(C - 1).start()

    for j in range(1, F):
        lgcopy(j, feat(j)).wait_recv()
    lt = lgbuf[0]
    for g in range(1, F):
        lt = lt + lgbuf[g]
    picked = jnp.zeros(ids.shape, F32)
    for e in range(E):
        picked = jnp.where(ids == e, lt[e : e + 1, :], picked)
    squashed = jax.nn.sigmoid(picked)
    gates = squashed / jnp.sum(squashed, axis=0, keepdims=True)
    gate_cols = [to_col(gates[k : k + 1, :]) for k in range(top)]

    def weighted(d):
        gd = jnp.zeros((T, 1), F32)
        for k in range(top):
            gd = gd + jnp.where(rel_cols[k] == d, gate_cols[k], 0.0)
        return gd * dot(place[d], ybuf[d])

    hid[...] = hid[...] + weighted(0)

    @pl.loop(1, C)
    def _(d):
        ycopy(d).wait_recv()
        hid[...] = hid[...] + weighted(d)

    out_ref[...] = hid[...].astype(BF16)

    @pl.loop(1, C - me)
    def _(d):
        kcopy(d).wait_send()
        vcopy(d).wait_send()

    for j in range(1, F):
        sscopy(j, f).wait_send()
        lgcopy(j, f).wait_send()

    @pl.loop(0, C)
    def _(d):
        for j in range(1, R):
            acopy(d, j, rep).wait_send()
            icopy(d, j, rep).wait_send()
        for j in range(1, S):
            bcopy(d, j, sec).wait_send()

    @pl.loop(1, C)
    def _(d):
        dcopy(d).wait_send()
        ccopy(d).wait_send()
        ycopy(d).wait_send()


def local(C, S, R, stream, q, k, v, ids, home, router, gain, w_gate, w_up, w_down):
    T, W = stream.shape
    top = ids.shape[1]
    H = W // HEAD_SIZE
    F = S * R
    E = router.shape[1]
    HID = w_gate.shape[2]
    HR = HID // R
    capacity = min(T, max(2, 5 * T * top // (4 * C)))
    cap = -(-capacity // 16) * 16
    e_rows = -(-E // 8) * 8
    lanes = -(-cap // 128) * 128
    DMA = pltpu.SemaphoreType.DMA
    vmem = pl.BlockSpec(memory_space=pltpu.VMEM)
    smem = pl.BlockSpec(memory_space=pltpu.SMEM)
    hbm = pl.BlockSpec(memory_space=pl.ANY)
    V = pltpu.VMEM
    return pl.pallas_call(
        functools.partial(body, C, S, R, cap),
        out_shape=jax.ShapeDtypeStruct((T, W), BF16),
        in_specs=[hbm] * 5 + [smem] + [hbm] * 5,
        out_specs=vmem,
        scratch_shapes=[
            V((T, W), BF16), V((T, W), BF16), V(k.shape, BF16), V(k.shape, BF16),
            V((top, T), jnp.int32), V((E, W), BF16), V((W,), BF16),
            V((W, HID), BF16), V((W, HID), BF16), V((HID, W), BF16),
            V((H * T, HEAD_SIZE), BF16),
            V((C, T, HEAD_SIZE), BF16), V((C, T, HEAD_SIZE), BF16),
            V((C, H * T, T), F32), V((H * T, T), F32), V((H * T, T), F32),
            V((H * T, HEAD_SIZE), F32),
            V((T, W), F32), V((T, W), BF16),
            V((F, 8, T), F32), V((F, e_rows, T), F32),
            V((C, T, cap), BF16), V((C, 8, lanes), F32), V((C, 8, lanes), F32),
            V((C, cap, W), BF16), V((C, cap, W), BF16),
            V((C, R, cap, 2 * HR), BF16), V((C, R, cap, 2 * HR), BF16),
            V((C, cap, 2 * HR), BF16), V((C, S, cap, 2 * HR), BF16),
            V((C, R, cap, HR), BF16),
            V((C, cap, W), BF16), V((C, cap, W), BF16),
            DMA((3,)), DMA((7,)), DMA((C,)), DMA((C,)),
            DMA((C,)), DMA((C,)), DMA((C,)), DMA((C,)),
            DMA((F,)), DMA((F,)), DMA((F,)), DMA((F,)),
            DMA((C,)), DMA((C,)),
            DMA((C, R)), DMA((C, R)),
            DMA((C, S)), DMA((C, S)),
            DMA((C, R)), DMA((C, R)),
            DMA((C,)), DMA((C,)),
        ],
        compiler_params=pltpu.CompilerParams(
            collective_id=0, has_side_effects=True, vmem_limit_bytes=62 * 1024 * 1024
        ),
        name="block",
    )(stream, q, k, v, ids.T, home, router.T, gain, w_gate, w_up, w_down)


def solution(mesh):
    placed = (
        P(("group", "ctx"), ("section", "rep")),
        P(("group", "ctx"), ("section", "rep")),
        P(("group", "ctx"), None),
        P(("group", "ctx"), None),
        P(("group", "ctx"), None),
        P(),
        P(("section", "rep"), None),
        P(("section", "rep")),
        P("ctx", ("section", "rep"), None),
        P("ctx", ("section", "rep"), None),
        P("ctx", None, ("section", "rep")),
    )
    return jax.shard_map(
        functools.partial(
            local, mesh.shape["ctx"], mesh.shape["section"], mesh.shape["rep"]
        ),
        mesh=mesh,
        in_specs=placed,
        out_specs=P(("group", "ctx"), ("section", "rep")),
        check_vma=False,
    )
```

```python
import functools
import math

import jax
import jax.numpy as jnp
from jax import lax
from jax.experimental import pallas as pl
from jax.experimental.pallas import tpu as pltpu
from jax.sharding import PartitionSpec as P

HEAD_SIZE = 128
epsilon = 1e-06
very_negative = -1e30
MESH = pl.DeviceIdType.MESH
F32 = jnp.float32
BF16 = jnp.bfloat16


def dot(a, b):
    return jnp.dot(a, b, preferred_element_type=F32)


def body(
    C, S, R, cap,
    stream_hbm, q_hbm, k_hbm, v_hbm, ids_hbm, home_ref, router_hbm, gain_hbm,
    wg_hbm, wu_hbm, wd_hbm,
    out_ref,
    stream_ref, q_ref, k_ref, v_ref, ids_ref, router_ref, gain_ref,
    wg, wu, wd, qs, kbuf, vbuf, sbuf, mbuf, lbuf, acc, hid, nrm, ssbuf, lgbuf,
    place, scsrc, scbuf, dsrc, dbuf, asrc, abuf, bsrc, bbuf, ibuf, ysrc, ybuf,
    w_sem, x_sem, kf_send, kf_recv, vf_send, vf_recv, c_send, c_recv, k_send, k_recv, v_send, v_recv, ss_send, ss_recv, lg_send, lg_recv,
    d_send, d_recv, a_send, a_recv, b_send, b_recv, i_send, i_recv, y_send, y_recv,
):
    T, W = stream_ref.shape
    H = W // HEAD_SIZE
    F = S * R
    E = router_ref.shape[0]
    HID = wg.shape[1]
    HR = HID // R
    top = ids_ref.shape[0]
    me = lax.axis_index("ctx")
    sec = lax.axis_index("section")
    rep = lax.axis_index("rep")
    f = sec * R + rep
    kv_heads = k_ref.shape[1] // HEAD_SIZE
    kv = f * H // (H * F // kv_heads)

    def ctx_dev(d):
        return {"ctx": lax.rem(me + d + C, C)}

    def feat(j):
        return lax.rem(f + j, F)

    def feat_dev(j):
        g = feat(j)
        return {"section": g // R, "rep": lax.rem(g, R)}

    def rc(src, dst, ss, rs, dev):
        return pltpu.make_async_remote_copy(
            src_ref=src, dst_ref=dst, send_sem=ss, recv_sem=rs,
            device_id=dev, device_id_type=MESH,
        )

    weights = [
        pltpu.make_async_copy(wg_hbm.at[0], wg, w_sem.at[0]),
        pltpu.make_async_copy(wu_hbm.at[0], wu, w_sem.at[1]),
        pltpu.make_async_copy(wd_hbm.at[0], wd, w_sem.at[2]),
    ]
    staged = [
        pltpu.make_async_copy(src, dst, x_sem.at[i])
        for i, (src, dst) in enumerate(
            (
                (k_hbm, k_ref), (v_hbm, v_ref), (q_hbm, q_ref), (ids_hbm, ids_ref),
                (stream_hbm, stream_ref), (gain_hbm, gain_ref), (router_hbm, router_ref),
            )
        )
    ]
    for c in staged:
        c.start()
    for c in weights:
        c.start()

    barrier = pltpu.get_barrier_semaphore()
    for d in range(1, C):
        pl.semaphore_signal(barrier, inc=1, device_id=ctx_dev(d), device_id_type=MESH)
    for j in range(1, F):
        pl.semaphore_signal(barrier, inc=1, device_id=feat_dev(j), device_id_type=MESH)
    staged[0].wait()
    staged[1].wait()
    pl.semaphore_wait(barrier, C - 1 + F - 1)

    kcols = pl.ds(pl.multiple_of(kv * HEAD_SIZE, HEAD_SIZE), HEAD_SIZE)

    shared = (H * F // kv_heads) % (H * R) == 0 and T % (16 * R) == 0
    RK = R if shared else 1
    TR = T // RK

    def share(owner):
        if RK == 1:
            return slice(None)
        return pl.ds(pl.multiple_of(owner * TR, TR), TR)

    def kcopy(d):
        rows = share(rep)
        return rc(
            k_ref.at[rows, kcols], kbuf.at[d, rows], k_send.at[d], k_recv.at[d], ctx_dev(d)
        )

    def vcopy(d):
        rows = share(rep)
        return rc(
            v_ref.at[rows, kcols], vbuf.at[d, rows], v_send.at[d], v_recv.at[d], ctx_dev(d)
        )

    def kforward(d, j, owner):
        part = kbuf.at[d, share(owner)]
        return rc(
            part, part, kf_send.at[d, j], kf_recv.at[d, owner], {"rep": lax.rem(rep + j, R)}
        )

    def vforward(d, j, owner):
        part = vbuf.at[d, share(owner)]
        return rc(
            part, part, vf_send.at[d, j], vf_recv.at[d, owner], {"rep": lax.rem(rep + j, R)}
        )

    @pl.loop(1, C - me)
    def _(d):
        kcopy(d).start()
        vcopy(d).start()

    for c in staged[2:]:
        c.wait()
    kbuf[0] = k_ref[:, kcols]
    vbuf[0] = v_ref[:, kcols]
    for h in range(H):
        qs[h * T : (h + 1) * T, :] = q_ref[:, h * HEAD_SIZE : (h + 1) * HEAD_SIZE]
    scale = 1.0 / math.sqrt(HEAD_SIZE)

    def scores(d):
        return (
            lax.dot_general(
                qs[...], kbuf[d], (((1,), (1,)), ((), ())), preferred_element_type=F32
            )
            * scale
        )

    row_t = lax.broadcasted_iota(jnp.int32, (T, T), 0)
    col_t = lax.broadcasted_iota(jnp.int32, (T, T), 1)
    s0 = scores(0)
    seen = jnp.concatenate([row_t >= col_t] * H, axis=0)
    s0 = jnp.where(seen, s0, very_negative)
    sbuf[0] = s0
    mbuf[...] = s0

    eye = row_t == col_t

    def to_row(col):
        return jnp.sum(jnp.where(eye, col, 0.0), axis=0, keepdims=True)

    def to_col(row):
        return jnp.sum(jnp.where(eye, row, 0.0), axis=1, keepdims=True)

    ids = ids_ref[...]
    dest = jnp.zeros_like(ids)
    for e in range(E):
        dest = jnp.where(ids == e, home_ref[e], dest)
    rel = dest - me
    rel = jnp.where(rel < 0, rel + C, rel)
    lanes = lax.broadcasted_iota(jnp.int32, (T, 128), 1)
    hot = jnp.zeros((T, 128), F32)
    rel_cols = [to_col(rel[k : k + 1, :].astype(F32)).astype(jnp.int32) for k in range(top)]
    for k in range(top):
        hot = hot + jnp.where(rel_cols[k] == lanes, 1.0, 0.0)
    lower = jnp.where(row_t > col_t, 1.0, 0.0).astype(BF16)
    rank = dot(lower, hot.astype(BF16))
    slots = lax.broadcasted_iota(jnp.int32, (T, cap), 1).astype(F32)
    for d in range(C):
        chosen = (hot[:, d : d + 1] > 0.5) & (rank[:, d : d + 1] == slots)
        place[d] = jnp.where(chosen, 1.0, 0.0).astype(BF16)

    def earlier_scores(d):
        for j in range(1, RK):
            kforward(d, j, lax.rem(rep + j, R)).wait_recv()
        s = scores(d)
        sbuf[d] = s
        mbuf[...] = jnp.maximum(mbuf[...], s)

    @pl.loop(1, me + 1)
    def _(d):
        kcopy(d).wait_recv()
        for j in range(1, RK):
            kforward(d, j, rep).start()
        vcopy(d).wait_recv()
        for j in range(1, RK):
            vforward(d, j, rep).start()

        @pl.when(d >= 2)
        def _():
            earlier_scores(d - 1)

    @pl.when(me >= 1)
    def _():
        earlier_scores(me)

    row_max = jnp.max(mbuf[...], axis=-1, keepdims=True)
    mbuf[...] = jnp.broadcast_to(row_max, mbuf.shape)
    e0 = jnp.exp(sbuf[0] - mbuf[...])
    lbuf[...] = e0
    acc[...] = dot(e0.astype(BF16), vbuf[0])

    @pl.loop(1, me + 1)
    def _(d):
        for j in range(1, RK):
            vforward(d, j, lax.rem(rep + j, R)).wait_recv()
        ex = jnp.exp(sbuf[d] - mbuf[...])
        lbuf[...] = lbuf[...] + ex
        acc[...] = acc[...] + dot(ex.astype(BF16), vbuf[d])

    sq = jnp.zeros((T, HEAD_SIZE), F32)
    for h in range(H):
        rows = slice(h * T, (h + 1) * T)
        cols = slice(h * HEAD_SIZE, (h + 1) * HEAD_SIZE)
        total = jnp.sum(lbuf[rows, :], axis=-1, keepdims=True)
        hv = stream_ref[:, cols].astype(F32) + acc[rows, :] / total
        hid[:, cols] = hv
        sq = sq + hv * hv
    ssbuf[f] = jnp.broadcast_to(to_row(jnp.sum(sq, axis=-1, keepdims=True)), (8, T))

    def sscopy(j, owner):
        return rc(ssbuf.at[owner], ssbuf.at[owner], ss_send.at[j], ss_recv.at[owner], feat_dev(j))

    def lgcopy(j, owner):
        return rc(lgbuf.at[owner], lgbuf.at[owner], lg_send.at[j], lg_recv.at[owner], feat_dev(j))

    for j in range(1, F):
        sscopy(j, f).start()
    gain = gain_ref[...].astype(F32).reshape(1, W)
    nrm[...] = (hid[...] * gain).astype(BF16)

    def dcopy(d):
        return rc(dsrc.at[d], dbuf.at[d], d_send.at[d], d_recv.at[d], ctx_dev(d))

    def gathered(d):
        return lax.dot_general(
            place[d], nrm[...], (((0,), (0,)), ((), ())), preferred_element_type=F32
        ).astype(BF16)

    @pl.loop(1, C)
    def _(d):
        dsrc[d] = gathered(d)
        dcopy(d).start()

    dbuf[0] = gathered(0)

    for c in weights:
        c.wait()

    def rep_at(j):
        return lax.rem(rep + j, R)

    def sec_at(j):
        return lax.rem(sec + j, S)

    def acopy(d, j, owner):
        return rc(
            asrc.at[d, rep_at(j)], abuf.at[d, owner], a_send.at[d, j], a_recv.at[d, owner],
            {"rep": rep_at(j)},
        )

    def bcopy(d, j, owner):
        return rc(
            bsrc.at[d], bbuf.at[d, owner], b_send.at[d, j], b_recv.at[d, owner],
            {"section": sec_at(j)},
        )

    def icopy(d, j, owner):
        return rc(
            ibuf.at[d, owner], ibuf.at[d, owner], i_send.at[d, j], i_recv.at[d, owner],
            {"rep": rep_at(j)},
        )

    def ycopy(d):
        return rc(ysrc.at[d], ybuf.at[d], y_send.at[d], y_recv.at[d], ctx_dev(-d))

    def stage_g(d):
        x = dbuf[d]
        for r in range(R):
            cols = slice(r * HR, (r + 1) * HR)
            asrc[d, r, :, 0:HR] = dot(x, wg[:, cols]).astype(BF16)
            asrc[d, r, :, HR : 2 * HR] = dot(x, wu[:, cols]).astype(BF16)
        for j in range(1, R):
            acopy(d, j, rep).start()

    def stage_b(d):
        total = asrc[d, rep].astype(F32)
        for j in range(1, R):
            acopy(d, j, rep_at(j)).wait_recv()
            total = total + abuf[d, rep_at(j)].astype(F32)
        bsrc[d] = total.astype(BF16)
        for j in range(1, S):
            bcopy(d, j, sec).start()

    eye_cap = lax.broadcasted_iota(jnp.int32, (cap, cap), 0) == lax.broadcasted_iota(
        jnp.int32, (cap, cap), 1
    )

    def ccopy(d):
        return rc(scsrc.at[d], scbuf.at[d], c_send.at[d], c_recv.at[d], ctx_dev(d))

    def rows_scale(d):
        return jnp.sum(jnp.where(eye_cap, scbuf[d, 0:1, 0:cap], 0.0), axis=1, keepdims=True)

    def stage_i(d):
        total = bsrc[d].astype(F32)
        for j in range(1, S):
            bcopy(d, j, sec_at(j)).wait_recv()
            total = total + bbuf[d, sec_at(j)].astype(F32)
        total = total * rows_scale(d)
        g = total[:, 0:HR]
        u = total[:, HR : 2 * HR]
        ibuf[d, rep] = (g * jax.nn.sigmoid(g) * u).astype(BF16)
        for j in range(1, R):
            icopy(d, j, rep).start()

    def stage_d(d):
        for j in range(1, R):
            icopy(d, j, rep_at(j)).wait_recv()
        y = dot(ibuf[d, 0], wd[0:HR, :])
        for r in range(1, R):
            y = y + dot(ibuf[d, r], wd[r * HR : (r + 1) * HR, :])
        return y.astype(BF16)

    stage_g(0)

    for j in range(1, F):
        sscopy(j, feat(j)).wait_recv()
    ss = ssbuf[0]
    for g in range(1, F):
        ss = ss + ssbuf[g]
    scale_rows = lax.rsqrt(to_col(ss[0:1, :]) / (W * F) + epsilon)

    def slot_scale(d):
        return jnp.sum(jnp.where(place[d].astype(F32) > 0.5, scale_rows, 0.0), axis=0, keepdims=True)

    @pl.loop(1, C)
    def _(d):
        scsrc[d, 0:1, 0:cap] = slot_scale(d)
        ccopy(d).start()

    scbuf[0, 0:1, 0:cap] = slot_scale(0)

    stage_b(0)

    normed = (hid[...] * scale_rows * gain).astype(BF16)
    lgbuf[f, 0:E, :] = lax.dot_general(
        router_ref[...], normed, (((1,), (1,)), ((), ())), preferred_element_type=F32
    )
    for j in range(1, F):
        lgcopy(j, f).start()

    if C > 1:
        dcopy(1).wait_recv()
        stage_g(1)
    stage_i(0)
    if C > 1:
        stage_b(1)
    ybuf[0] = stage_d(0)

    @pl.loop(2, C)
    def _(d):
        dcopy(d).wait_recv()
        stage_g(d)
        ccopy(d - 1).wait_recv()
        stage_i(d - 1)
        stage_b(d)
        ysrc[d - 1] = stage_d(d - 1)
        ycopy(d - 1).start()

    if C > 1:
        ccopy(C - 1).wait_recv()
        stage_i(C - 1)
        ysrc[C - 1] = stage_d(C - 1)
        ycopy(C - 1).start()

    for j in range(1, F):
        lgcopy(j, feat(j)).wait_recv()
    lt = lgbuf[0]
    for g in range(1, F):
        lt = lt + lgbuf[g]
    picked = jnp.zeros(ids.shape, F32)
    for e in range(E):
        picked = jnp.where(ids == e, lt[e : e + 1, :], picked)
    squashed = jax.nn.sigmoid(picked)
    gates = squashed / jnp.sum(squashed, axis=0, keepdims=True)
    gate_cols = [to_col(gates[k : k + 1, :]) for k in range(top)]

    def weighted(d):
        gd = jnp.zeros((T, 1), F32)
        for k in range(top):
            gd = gd + jnp.where(rel_cols[k] == d, gate_cols[k], 0.0)
        return gd * dot(place[d], ybuf[d])

    hid[...] = hid[...] + weighted(0)

    @pl.loop(1, C)
    def _(d):
        ycopy(d).wait_recv()
        hid[...] = hid[...] + weighted(d)

    out_ref[...] = hid[...].astype(BF16)

    @pl.loop(1, C - me)
    def _(d):
        kcopy(d).wait_send()
        vcopy(d).wait_send()

    @pl.loop(1, me + 1)
    def _(d):
        for j in range(1, RK):
            kforward(d, j, rep).wait_send()
            vforward(d, j, rep).wait_send()

    for j in range(1, F):
        sscopy(j, f).wait_send()
        lgcopy(j, f).wait_send()

    @pl.loop(0, C)
    def _(d):
        for j in range(1, R):
            acopy(d, j, rep).wait_send()
            icopy(d, j, rep).wait_send()
        for j in range(1, S):
            bcopy(d, j, sec).wait_send()

    @pl.loop(1, C)
    def _(d):
        dcopy(d).wait_send()
        ccopy(d).wait_send()
        ycopy(d).wait_send()


def local(C, S, R, stream, q, k, v, ids, home, router, gain, w_gate, w_up, w_down):
    T, W = stream.shape
    top = ids.shape[1]
    H = W // HEAD_SIZE
    F = S * R
    E = router.shape[1]
    HID = w_gate.shape[2]
    HR = HID // R
    capacity = min(T, max(2, 5 * T * top // (4 * C)))
    cap = -(-capacity // 16) * 16
    e_rows = -(-E // 8) * 8
    lanes = -(-cap // 128) * 128
    DMA = pltpu.SemaphoreType.DMA
    vmem = pl.BlockSpec(memory_space=pltpu.VMEM)
    smem = pl.BlockSpec(memory_space=pltpu.SMEM)
    hbm = pl.BlockSpec(memory_space=pltpu.HBM)
    V = pltpu.VMEM
    scratch = [
        V((T, W), BF16), V((T, W), BF16), V(k.shape, BF16), V(k.shape, BF16),
        V((top, T), jnp.int32), V((E, W), BF16), V((W,), BF16),
        V((W, HID), BF16), V((W, HID), BF16), V((HID, W), BF16),
        V((H * T, HEAD_SIZE), BF16),
        V((C, T, HEAD_SIZE), BF16), V((C, T, HEAD_SIZE), BF16),
        V((C, H * T, T), F32), V((H * T, T), F32), V((H * T, T), F32),
        V((H * T, HEAD_SIZE), F32),
        V((T, W), F32), V((T, W), BF16),
        V((F, 8, T), F32), V((F, e_rows, T), F32),
        V((C, T, cap), BF16), V((C, 8, lanes), F32), V((C, 8, lanes), F32),
        V((C, cap, W), BF16), V((C, cap, W), BF16),
        V((C, R, cap, 2 * HR), BF16), V((C, R, cap, 2 * HR), BF16),
        V((C, cap, 2 * HR), BF16), V((C, S, cap, 2 * HR), BF16),
        V((C, R, cap, HR), BF16),
        V((C, cap, W), BF16), V((C, cap, W), BF16),
        DMA((3,)), DMA((7,)), DMA((C, R)), DMA((C, R)), DMA((C, R)), DMA((C, R)), DMA((C,)), DMA((C,)),
        DMA((C,)), DMA((C,)), DMA((C,)), DMA((C,)),
        DMA((F,)), DMA((F,)), DMA((F,)), DMA((F,)),
        DMA((C,)), DMA((C,)),
        DMA((C, R)), DMA((C, R)),
        DMA((C, S)), DMA((C, S)),
        DMA((C, R)), DMA((C, R)),
        DMA((C,)), DMA((C,)),
    ]
    used = sum(
        math.prod(x.shape) * jnp.dtype(x.dtype).itemsize for x in scratch if x.dtype in (F32, BF16)
    )
    limit = 62 << 20
    return pl.pallas_call(
        functools.partial(body, C, S, R, cap),
        out_shape=jax.ShapeDtypeStruct((T, W), BF16),
        in_specs=[hbm] * 5 + [smem] + [hbm] * 5,
        out_specs=vmem,
        scratch_shapes=scratch,
        compiler_params=pltpu.CompilerParams(
            collective_id=0, has_side_effects=True, vmem_limit_bytes=limit
        ),
        name="block",
    )(stream, q, k, v, ids.T, home, router.T, gain, w_gate, w_up, w_down)


def solution(mesh):
    placed = (
        P(("group", "ctx"), ("section", "rep")),
        P(("group", "ctx"), ("section", "rep")),
        P(("group", "ctx"), None),
        P(("group", "ctx"), None),
        P(("group", "ctx"), None),
        P(),
        P(("section", "rep"), None),
        P(("section", "rep")),
        P("ctx", ("section", "rep"), None),
        P("ctx", ("section", "rep"), None),
        P("ctx", None, ("section", "rep")),
    )
    return jax.shard_map(
        functools.partial(
            local, mesh.shape["ctx"], mesh.shape["section"], mesh.shape["rep"]
        ),
        mesh=mesh,
        in_specs=placed,
        out_specs=P(("group", "ctx"), ("section", "rep")),
        check_vma=False,
    )
```

```python
import functools
import math

import jax
import jax.numpy as jnp
from jax import lax
from jax.experimental import pallas as pl
from jax.experimental.pallas import tpu as pltpu
from jax.sharding import PartitionSpec as P

HEAD_SIZE = 128
epsilon = 1e-06
very_negative = -1e30
MESH = pl.DeviceIdType.MESH
F32 = jnp.float32
BF16 = jnp.bfloat16


def dot(a, b):
    return jnp.dot(a, b, preferred_element_type=F32)


def body(
    C, S, R, cap,
    stream_hbm, q_hbm, k_hbm, v_hbm, ids_hbm, home_ref, router_hbm, gain_hbm,
    wg_hbm, wu_hbm, wd_hbm,
    out_ref,
    stream_ref, q_ref, k_ref, v_ref, ids_ref, router_ref, gain_ref,
    wg, wu, wd, qs, kbuf, vbuf, sbuf, mbuf, lbuf, acc, hid, nrm, ssbuf, lgbuf,
    place, scsrc, scbuf, dsrc, dbuf, asrc, abuf, bsrc, bbuf, ibuf, ysrc, ybuf,
    w_sem, x_sem, kf_send, kf_recv, vf_send, vf_recv, c_send, c_recv, k_send, k_recv, v_send, v_recv, ss_send, ss_recv, lg_send, lg_recv,
    d_send, d_recv, a_send, a_recv, b_send, b_recv, i_send, i_recv, y_send, y_recv,
):
    T, W = stream_ref.shape
    H = W // HEAD_SIZE
    F = S * R
    E = router_ref.shape[0]
    HID = wg.shape[1]
    HR = HID // R
    top = ids_ref.shape[0]
    me = lax.axis_index("ctx")
    sec = lax.axis_index("section")
    rep = lax.axis_index("rep")
    f = sec * R + rep
    kv_heads = k_ref.shape[1] // HEAD_SIZE
    kv = f * H // (H * F // kv_heads)

    def ctx_dev(d):
        return {"ctx": lax.rem(me + d + C, C)}

    def feat(j):
        return lax.rem(f + j, F)

    def feat_dev(j):
        g = feat(j)
        return {"section": g // R, "rep": lax.rem(g, R)}

    def other(i):
        return i - 1 + lax.div(i - 1 + C - me, C)

    def from_slot(i):
        return lax.rem(me - other(i) + C, C)

    def back_slot(i):
        return lax.rem(other(i) - me + C, C)

    def rc(src, dst, ss, rs, dev):
        return pltpu.make_async_remote_copy(
            src_ref=src, dst_ref=dst, send_sem=ss, recv_sem=rs,
            device_id=dev, device_id_type=MESH,
        )

    weights = [
        pltpu.make_async_copy(wg_hbm.at[0], wg, w_sem.at[0]),
        pltpu.make_async_copy(wu_hbm.at[0], wu, w_sem.at[1]),
        pltpu.make_async_copy(wd_hbm.at[0], wd, w_sem.at[2]),
    ]
    staged = [
        pltpu.make_async_copy(src, dst, x_sem.at[i])
        for i, (src, dst) in enumerate(
            (
                (k_hbm, k_ref), (v_hbm, v_ref), (q_hbm, q_ref), (ids_hbm, ids_ref),
                (stream_hbm, stream_ref), (gain_hbm, gain_ref), (router_hbm, router_ref),
            )
        )
    ]
    for c in staged:
        c.start()
    for c in weights:
        c.start()

    barrier = pltpu.get_barrier_semaphore()
    for d in range(1, C):
        pl.semaphore_signal(barrier, inc=1, device_id=ctx_dev(d), device_id_type=MESH)
    for j in range(1, F):
        pl.semaphore_signal(barrier, inc=1, device_id=feat_dev(j), device_id_type=MESH)
    staged[0].wait()
    staged[1].wait()
    pl.semaphore_wait(barrier, C - 1 + F - 1)

    kcols = pl.ds(pl.multiple_of(kv * HEAD_SIZE, HEAD_SIZE), HEAD_SIZE)

    shared = (H * F // kv_heads) % (H * R) == 0 and T % (16 * R) == 0
    RK = R if shared else 1
    TR = T // RK

    def share(owner):
        if RK == 1:
            return slice(None)
        return pl.ds(pl.multiple_of(owner * TR, TR), TR)

    def kcopy(d):
        rows = share(rep)
        return rc(
            k_ref.at[rows, kcols], kbuf.at[d, rows], k_send.at[d], k_recv.at[d], ctx_dev(d)
        )

    def vcopy(d):
        rows = share(rep)
        return rc(
            v_ref.at[rows, kcols], vbuf.at[d, rows], v_send.at[d], v_recv.at[d], ctx_dev(d)
        )

    def kforward(d, j, owner):
        part = kbuf.at[d, share(owner)]
        return rc(
            part, part, kf_send.at[d, j], kf_recv.at[d, owner], {"rep": lax.rem(rep + j, R)}
        )

    def vforward(d, j, owner):
        part = vbuf.at[d, share(owner)]
        return rc(
            part, part, vf_send.at[d, j], vf_recv.at[d, owner], {"rep": lax.rem(rep + j, R)}
        )

    @pl.loop(1, C - me)
    def _(d):
        kcopy(d).start()
        vcopy(d).start()

    for c in staged[2:]:
        c.wait()
    kbuf[0] = k_ref[:, kcols]
    vbuf[0] = v_ref[:, kcols]
    for h in range(H):
        qs[h * T : (h + 1) * T, :] = q_ref[:, h * HEAD_SIZE : (h + 1) * HEAD_SIZE]
    scale = 1.0 / math.sqrt(HEAD_SIZE)

    def scores(d):
        return (
            lax.dot_general(
                qs[...], kbuf[d], (((1,), (1,)), ((), ())), preferred_element_type=F32
            )
            * scale
        )

    row_t = lax.broadcasted_iota(jnp.int32, (T, T), 0)
    col_t = lax.broadcasted_iota(jnp.int32, (T, T), 1)
    s0 = scores(0)
    seen = jnp.concatenate([row_t >= col_t] * H, axis=0)
    s0 = jnp.where(seen, s0, very_negative)
    sbuf[0] = s0
    mbuf[...] = s0

    eye = row_t == col_t

    def to_row(col):
        return jnp.sum(jnp.where(eye, col, 0.0), axis=0, keepdims=True)

    def to_col(row):
        return jnp.sum(jnp.where(eye, row, 0.0), axis=1, keepdims=True)

    ids = ids_ref[...]
    dest = jnp.zeros_like(ids)
    for e in range(E):
        dest = jnp.where(ids == e, home_ref[e], dest)
    rel = dest - me
    rel = jnp.where(rel < 0, rel + C, rel)
    lanes = lax.broadcasted_iota(jnp.int32, (T, 128), 1)
    hot = jnp.zeros((T, 128), F32)
    rel_cols = [to_col(rel[k : k + 1, :].astype(F32)).astype(jnp.int32) for k in range(top)]
    for k in range(top):
        hot = hot + jnp.where(rel_cols[k] == lanes, 1.0, 0.0)
    lower = jnp.where(row_t > col_t, 1.0, 0.0).astype(BF16)
    rank = dot(lower, hot.astype(BF16))
    slots = lax.broadcasted_iota(jnp.int32, (T, cap), 1).astype(F32)
    for d in range(C):
        chosen = (hot[:, d : d + 1] > 0.5) & (rank[:, d : d + 1] == slots)
        place[d] = jnp.where(chosen, 1.0, 0.0).astype(BF16)

    def earlier_scores(d):
        for j in range(1, RK):
            kforward(d, j, lax.rem(rep + j, R)).wait_recv()
        s = scores(d)
        sbuf[d] = s
        mbuf[...] = jnp.maximum(mbuf[...], s)

    @pl.loop(1, me + 1)
    def _(d):
        kcopy(d).wait_recv()
        for j in range(1, RK):
            kforward(d, j, rep).start()
        vcopy(d).wait_recv()
        for j in range(1, RK):
            vforward(d, j, rep).start()

        @pl.when(d >= 2)
        def _():
            earlier_scores(d - 1)

    @pl.when(me >= 1)
    def _():
        earlier_scores(me)

    row_max = jnp.max(mbuf[...], axis=-1, keepdims=True)
    mbuf[...] = jnp.broadcast_to(row_max, mbuf.shape)
    e0 = jnp.exp(sbuf[0] - mbuf[...])
    lbuf[...] = e0
    acc[...] = dot(e0.astype(BF16), vbuf[0])

    @pl.loop(1, me + 1)
    def _(d):
        for j in range(1, RK):
            vforward(d, j, lax.rem(rep + j, R)).wait_recv()
        ex = jnp.exp(sbuf[d] - mbuf[...])
        lbuf[...] = lbuf[...] + ex
        acc[...] = acc[...] + dot(ex.astype(BF16), vbuf[d])

    sq = jnp.zeros((T, HEAD_SIZE), F32)
    for h in range(H):
        rows = slice(h * T, (h + 1) * T)
        cols = slice(h * HEAD_SIZE, (h + 1) * HEAD_SIZE)
        total = jnp.sum(lbuf[rows, :], axis=-1, keepdims=True)
        hv = stream_ref[:, cols].astype(F32) + acc[rows, :] / total
        hid[:, cols] = hv
        sq = sq + hv * hv
    ssbuf[f] = jnp.broadcast_to(to_row(jnp.sum(sq, axis=-1, keepdims=True)), (8, T))

    def sscopy(j, owner):
        return rc(ssbuf.at[owner], ssbuf.at[owner], ss_send.at[j], ss_recv.at[owner], feat_dev(j))

    def lgcopy(j, owner):
        return rc(lgbuf.at[owner], lgbuf.at[owner], lg_send.at[j], lg_recv.at[owner], feat_dev(j))

    for j in range(1, F):
        sscopy(j, f).start()
    gain = gain_ref[...].astype(F32).reshape(1, W)
    nrm[...] = (hid[...] * gain).astype(BF16)

    def dcopy(d):
        return rc(dsrc.at[d], dbuf.at[d], d_send.at[d], d_recv.at[d], ctx_dev(d))

    def gathered(d):
        return lax.dot_general(
            place[d], nrm[...], (((0,), (0,)), ((), ())), preferred_element_type=F32
        ).astype(BF16)

    @pl.loop(1, C)
    def _(d):
        dsrc[d] = gathered(d)
        dcopy(d).start()

    dbuf[0] = gathered(0)

    for c in weights:
        c.wait()

    def rep_at(j):
        return lax.rem(rep + j, R)

    def sec_at(j):
        return lax.rem(sec + j, S)

    def acopy(d, j, owner):
        return rc(
            asrc.at[d, rep_at(j)], abuf.at[d, owner], a_send.at[d, j], a_recv.at[d, owner],
            {"rep": rep_at(j)},
        )

    def bcopy(d, j, owner):
        return rc(
            bsrc.at[d], bbuf.at[d, owner], b_send.at[d, j], b_recv.at[d, owner],
            {"section": sec_at(j)},
        )

    def icopy(d, j, owner):
        return rc(
            ibuf.at[d, owner], ibuf.at[d, owner], i_send.at[d, j], i_recv.at[d, owner],
            {"rep": rep_at(j)},
        )

    def ycopy(d):
        return rc(ysrc.at[d], ybuf.at[d], y_send.at[d], y_recv.at[d], ctx_dev(-d))

    def stage_g(d):
        x = dbuf[d]
        for r in range(R):
            cols = slice(r * HR, (r + 1) * HR)
            asrc[d, r, :, 0:HR] = dot(x, wg[:, cols]).astype(BF16)
            asrc[d, r, :, HR : 2 * HR] = dot(x, wu[:, cols]).astype(BF16)
        for j in range(1, R):
            acopy(d, j, rep).start()

    def stage_b(d):
        total = asrc[d, rep].astype(F32)
        for j in range(1, R):
            acopy(d, j, rep_at(j)).wait_recv()
            total = total + abuf[d, rep_at(j)].astype(F32)
        bsrc[d] = total.astype(BF16)
        for j in range(1, S):
            bcopy(d, j, sec).start()

    eye_cap = lax.broadcasted_iota(jnp.int32, (cap, cap), 0) == lax.broadcasted_iota(
        jnp.int32, (cap, cap), 1
    )

    def ccopy(d):
        return rc(scsrc.at[d], scbuf.at[d], c_send.at[d], c_recv.at[d], ctx_dev(d))

    def rows_scale(d):
        return jnp.sum(jnp.where(eye_cap, scbuf[d, 0:1, 0:cap], 0.0), axis=1, keepdims=True)

    def stage_i(d):
        total = bsrc[d].astype(F32)
        for j in range(1, S):
            bcopy(d, j, sec_at(j)).wait_recv()
            total = total + bbuf[d, sec_at(j)].astype(F32)
        total = total * rows_scale(d)
        g = total[:, 0:HR]
        u = total[:, HR : 2 * HR]
        ibuf[d, rep] = (g * jax.nn.sigmoid(g) * u).astype(BF16)
        for j in range(1, R):
            icopy(d, j, rep).start()

    def stage_d(d):
        for j in range(1, R):
            icopy(d, j, rep_at(j)).wait_recv()
        y = dot(ibuf[d, 0], wd[0:HR, :])
        for r in range(1, R):
            y = y + dot(ibuf[d, r], wd[r * HR : (r + 1) * HR, :])
        return y.astype(BF16)

    stage_g(0)

    for j in range(1, F):
        sscopy(j, feat(j)).wait_recv()
    ss = ssbuf[0]
    for g in range(1, F):
        ss = ss + ssbuf[g]
    scale_rows = lax.rsqrt(to_col(ss[0:1, :]) / (W * F) + epsilon)

    def slot_scale(d):
        return jnp.sum(jnp.where(place[d].astype(F32) > 0.5, scale_rows, 0.0), axis=0, keepdims=True)

    @pl.loop(1, C)
    def _(d):
        scsrc[d, 0:1, 0:cap] = slot_scale(d)
        ccopy(d).start()

    scbuf[0, 0:1, 0:cap] = slot_scale(0)

    stage_b(0)

    normed = (hid[...] * scale_rows * gain).astype(BF16)
    lgbuf[f, 0:E, :] = lax.dot_general(
        router_ref[...], normed, (((1,), (1,)), ((), ())), preferred_element_type=F32
    )
    for j in range(1, F):
        lgcopy(j, f).start()

    if C > 1:
        first = from_slot(1)
        dcopy(first).wait_recv()
        stage_g(first)
    stage_i(0)
    if C > 1:
        stage_b(first)
    ybuf[0] = stage_d(0)

    def give_back(d):
        ysrc[d] = stage_d(d)
        ycopy(d).start()

    @pl.loop(2, C)
    def _(i):
        d = from_slot(i)
        before = from_slot(i - 1)
        dcopy(d).wait_recv()
        stage_g(d)
        ccopy(before).wait_recv()
        stage_i(before)
        stage_b(d)
        give_back(before)

    if C > 1:
        last = from_slot(C - 1)
        ccopy(last).wait_recv()
        stage_i(last)
        give_back(last)

    for j in range(1, F):
        lgcopy(j, feat(j)).wait_recv()
    lt = lgbuf[0]
    for g in range(1, F):
        lt = lt + lgbuf[g]
    picked = jnp.zeros(ids.shape, F32)
    for e in range(E):
        picked = jnp.where(ids == e, lt[e : e + 1, :], picked)
    squashed = jax.nn.sigmoid(picked)
    gates = squashed / jnp.sum(squashed, axis=0, keepdims=True)
    gate_cols = [to_col(gates[k : k + 1, :]) for k in range(top)]

    def weighted(d):
        gd = jnp.zeros((T, 1), F32)
        for k in range(top):
            gd = gd + jnp.where(rel_cols[k] == d, gate_cols[k], 0.0)
        return gd * dot(place[d], ybuf[d])

    hid[...] = hid[...] + weighted(0)

    @pl.loop(1, C)
    def _(i):
        d = back_slot(i)
        ycopy(d).wait_recv()
        hid[...] = hid[...] + weighted(d)

    out_ref[...] = hid[...].astype(BF16)

    @pl.loop(1, C - me)
    def _(d):
        kcopy(d).wait_send()
        vcopy(d).wait_send()

    @pl.loop(1, me + 1)
    def _(d):
        for j in range(1, RK):
            kforward(d, j, rep).wait_send()
            vforward(d, j, rep).wait_send()

    for j in range(1, F):
        sscopy(j, f).wait_send()
        lgcopy(j, f).wait_send()

    @pl.loop(0, C)
    def _(d):
        for j in range(1, R):
            acopy(d, j, rep).wait_send()
            icopy(d, j, rep).wait_send()
        for j in range(1, S):
            bcopy(d, j, sec).wait_send()

    @pl.loop(1, C)
    def _(d):
        dcopy(d).wait_send()
        ccopy(d).wait_send()
        ycopy(d).wait_send()


def local(C, S, R, stream, q, k, v, ids, home, router, gain, w_gate, w_up, w_down):
    T, W = stream.shape
    top = ids.shape[1]
    H = W // HEAD_SIZE
    F = S * R
    E = router.shape[1]
    HID = w_gate.shape[2]
    HR = HID // R
    capacity = min(T, max(2, 5 * T * top // (4 * C)))
    cap = -(-capacity // 16) * 16
    e_rows = -(-E // 8) * 8
    lanes = -(-cap // 128) * 128
    DMA = pltpu.SemaphoreType.DMA
    vmem = pl.BlockSpec(memory_space=pltpu.VMEM)
    smem = pl.BlockSpec(memory_space=pltpu.SMEM)
    hbm = pl.BlockSpec(memory_space=pltpu.HBM)
    V = pltpu.VMEM
    scratch = [
        V((T, W), BF16), V((T, W), BF16), V(k.shape, BF16), V(k.shape, BF16),
        V((top, T), jnp.int32), V((E, W), BF16), V((W,), BF16),
        V((W, HID), BF16), V((W, HID), BF16), V((HID, W), BF16),
        V((H * T, HEAD_SIZE), BF16),
        V((C, T, HEAD_SIZE), BF16), V((C, T, HEAD_SIZE), BF16),
        V((C, H * T, T), F32), V((H * T, T), F32), V((H * T, T), F32),
        V((H * T, HEAD_SIZE), F32),
        V((T, W), F32), V((T, W), BF16),
        V((F, 8, T), F32), V((F, e_rows, T), F32),
        V((C, T, cap), BF16), V((C, 8, lanes), F32), V((C, 8, lanes), F32),
        V((C, cap, W), BF16), V((C, cap, W), BF16),
        V((C, R, cap, 2 * HR), BF16), V((C, R, cap, 2 * HR), BF16),
        V((C, cap, 2 * HR), BF16), V((C, S, cap, 2 * HR), BF16),
        V((C, R, cap, HR), BF16),
        V((C, cap, W), BF16), V((C, cap, W), BF16),
        DMA((3,)), DMA((7,)), DMA((C, R)), DMA((C, R)), DMA((C, R)), DMA((C, R)), DMA((C,)), DMA((C,)),
        DMA((C,)), DMA((C,)), DMA((C,)), DMA((C,)),
        DMA((F,)), DMA((F,)), DMA((F,)), DMA((F,)),
        DMA((C,)), DMA((C,)),
        DMA((C, R)), DMA((C, R)),
        DMA((C, S)), DMA((C, S)),
        DMA((C, R)), DMA((C, R)),
        DMA((C,)), DMA((C,)),
    ]
    used = sum(
        math.prod(x.shape) * jnp.dtype(x.dtype).itemsize for x in scratch if x.dtype in (F32, BF16)
    )
    limit = 62 << 20
    return pl.pallas_call(
        functools.partial(body, C, S, R, cap),
        out_shape=jax.ShapeDtypeStruct((T, W), BF16),
        in_specs=[hbm] * 5 + [smem] + [hbm] * 5,
        out_specs=vmem,
        scratch_shapes=scratch,
        compiler_params=pltpu.CompilerParams(
            collective_id=0, has_side_effects=True, vmem_limit_bytes=limit
        ),
        name="block",
    )(stream, q, k, v, ids.T, home, router.T, gain, w_gate, w_up, w_down)


def solution(mesh):
    placed = (
        P(("group", "ctx"), ("section", "rep")),
        P(("group", "ctx"), ("section", "rep")),
        P(("group", "ctx"), None),
        P(("group", "ctx"), None),
        P(("group", "ctx"), None),
        P(),
        P(("section", "rep"), None),
        P(("section", "rep")),
        P("ctx", ("section", "rep"), None),
        P("ctx", ("section", "rep"), None),
        P("ctx", None, ("section", "rep")),
    )
    return jax.shard_map(
        functools.partial(
            local, mesh.shape["ctx"], mesh.shape["section"], mesh.shape["rep"]
        ),
        mesh=mesh,
        in_specs=placed,
        out_specs=P(("group", "ctx"), ("section", "rep")),
        check_vma=False,
    )
```

```python
import functools
import math

import jax
import jax.numpy as jnp
from jax import lax
from jax.experimental import pallas as pl
from jax.experimental.pallas import tpu as pltpu
from jax.sharding import PartitionSpec as P

HEAD_SIZE = 128
epsilon = 1e-06
very_negative = -1e30
MESH = pl.DeviceIdType.MESH
F32 = jnp.float32
BF16 = jnp.bfloat16


def dot(a, b):
    return jnp.dot(a, b, preferred_element_type=F32)


def body(
    C, S, R, cap,
    stream_hbm, q_hbm, k_hbm, v_hbm, ids_hbm, home_ref, router_hbm, gain_hbm,
    wg_hbm, wu_hbm, wd_hbm,
    out_ref,
    stream_ref, q_ref, k_ref, v_ref, ids_ref, router_ref, gain_ref,
    wg, wu, wd, qs, kbuf, vbuf, sbuf, mbuf, lbuf, acc, hid, nrm, ssbuf, lgbuf,
    place, scsrc, scbuf, dsrc, dbuf, asrc, abuf, bsrc, bbuf, ibuf, ysrc, ybuf,
    w_sem, x_sem, kf_send, kf_recv, vf_send, vf_recv, c_send, c_recv, k_send, k_recv, v_send, v_recv, ss_send, ss_recv, lg_send, lg_recv,
    d_send, d_recv, a_send, a_recv, b_send, b_recv, i_send, i_recv, y_send, y_recv,
):
    T, W = stream_ref.shape
    H = W // HEAD_SIZE
    F = S * R
    E = router_ref.shape[0]
    HID = wg.shape[1]
    HR = HID // R
    top = ids_ref.shape[0]
    me = lax.axis_index("ctx")
    sec = lax.axis_index("section")
    rep = lax.axis_index("rep")
    f = sec * R + rep
    kv_heads = k_ref.shape[1] // HEAD_SIZE
    kv = f * H // (H * F // kv_heads)

    def ctx_dev(d):
        return {"ctx": lax.rem(me + d + C, C)}

    def feat(j):
        return lax.rem(f + j, F)

    def feat_dev(j):
        g = feat(j)
        return {"section": g // R, "rep": lax.rem(g, R)}

    def rc(src, dst, ss, rs, dev):
        return pltpu.make_async_remote_copy(
            src_ref=src, dst_ref=dst, send_sem=ss, recv_sem=rs,
            device_id=dev, device_id_type=MESH,
        )

    weights = [
        pltpu.make_async_copy(wg_hbm.at[0], wg, w_sem.at[0]),
        pltpu.make_async_copy(wu_hbm.at[0], wu, w_sem.at[1]),
        pltpu.make_async_copy(wd_hbm.at[0], wd, w_sem.at[2]),
    ]
    staged = [
        pltpu.make_async_copy(src, dst, x_sem.at[i])
        for i, (src, dst) in enumerate(
            (
                (k_hbm, k_ref), (v_hbm, v_ref), (q_hbm, q_ref), (ids_hbm, ids_ref),
                (stream_hbm, stream_ref), (gain_hbm, gain_ref), (router_hbm, router_ref),
            )
        )
    ]
    for c in staged:
        c.start()
    for c in weights:
        c.start()

    barrier = pltpu.get_barrier_semaphore()
    for d in range(1, C):
        pl.semaphore_signal(barrier, inc=1, device_id=ctx_dev(d), device_id_type=MESH)
    for j in range(1, F):
        pl.semaphore_signal(barrier, inc=1, device_id=feat_dev(j), device_id_type=MESH)
    staged[0].wait()
    staged[1].wait()
    pl.semaphore_wait(barrier, C - 1 + F - 1)

    kcols = pl.ds(pl.multiple_of(kv * HEAD_SIZE, HEAD_SIZE), HEAD_SIZE)

    shared = (H * F // kv_heads) % (H * R) == 0 and T % (16 * R) == 0
    RK = R if shared else 1
    TR = T // RK

    def share(owner):
        if RK == 1:
            return slice(None)
        return pl.ds(pl.multiple_of(owner * TR, TR), TR)

    def kcopy(d):
        rows = share(rep)
        return rc(
            k_ref.at[rows, kcols], kbuf.at[d, rows], k_send.at[d], k_recv.at[d], ctx_dev(d)
        )

    def vcopy(d):
        rows = share(rep)
        return rc(
            v_ref.at[rows, kcols], vbuf.at[d, rows], v_send.at[d], v_recv.at[d], ctx_dev(d)
        )

    def kforward(d, j, owner):
        part = kbuf.at[d, share(owner)]
        return rc(
            part, part, kf_send.at[d, j], kf_recv.at[d, owner], {"rep": lax.rem(rep + j, R)}
        )

    def vforward(d, j, owner):
        part = vbuf.at[d, share(owner)]
        return rc(
            part, part, vf_send.at[d, j], vf_recv.at[d, owner], {"rep": lax.rem(rep + j, R)}
        )

    @pl.loop(1, C - me)
    def _(d):
        kcopy(d).start()
        vcopy(d).start()

    for c in staged[2:]:
        c.wait()
    kbuf[0] = k_ref[:, kcols]
    vbuf[0] = v_ref[:, kcols]
    for h in range(H):
        qs[h * T : (h + 1) * T, :] = q_ref[:, h * HEAD_SIZE : (h + 1) * HEAD_SIZE]
    scale = 1.0 / math.sqrt(HEAD_SIZE)

    def scores(d):
        return (
            lax.dot_general(
                qs[...], kbuf[d], (((1,), (1,)), ((), ())), preferred_element_type=F32
            )
            * scale
        )

    row_t = lax.broadcasted_iota(jnp.int32, (T, T), 0)
    col_t = lax.broadcasted_iota(jnp.int32, (T, T), 1)
    s0 = scores(0)
    seen = jnp.concatenate([row_t >= col_t] * H, axis=0)
    s0 = jnp.where(seen, s0, very_negative)
    sbuf[0] = s0
    mbuf[...] = s0

    eye = row_t == col_t

    def to_row(col):
        return jnp.sum(jnp.where(eye, col, 0.0), axis=0, keepdims=True)

    def to_col(row):
        return jnp.sum(jnp.where(eye, row, 0.0), axis=1, keepdims=True)

    ids = ids_ref[...]
    dest = jnp.zeros_like(ids)
    for e in range(E):
        dest = jnp.where(ids == e, home_ref[e], dest)
    rel = dest - me
    rel = jnp.where(rel < 0, rel + C, rel)
    lanes = lax.broadcasted_iota(jnp.int32, (T, 128), 1)
    hot = jnp.zeros((T, 128), F32)
    rel_cols = [to_col(rel[k : k + 1, :].astype(F32)).astype(jnp.int32) for k in range(top)]
    for k in range(top):
        hot = hot + jnp.where(rel_cols[k] == lanes, 1.0, 0.0)
    lower = jnp.where(row_t > col_t, 1.0, 0.0).astype(BF16)
    rank = dot(lower, hot.astype(BF16))
    slots = lax.broadcasted_iota(jnp.int32, (T, cap), 1).astype(F32)
    for d in range(C):
        chosen = (hot[:, d : d + 1] > 0.5) & (rank[:, d : d + 1] == slots)
        place[d] = jnp.where(chosen, 1.0, 0.0).astype(BF16)

    def earlier_scores(d):
        for j in range(1, RK):
            kforward(d, j, lax.rem(rep + j, R)).wait_recv()
        s = scores(d)
        sbuf[d] = s
        mbuf[...] = jnp.maximum(mbuf[...], s)

    @pl.loop(1, me + 1)
    def _(d):
        kcopy(d).wait_recv()
        for j in range(1, RK):
            kforward(d, j, rep).start()
        vcopy(d).wait_recv()
        for j in range(1, RK):
            vforward(d, j, rep).start()

        @pl.when(d >= 2)
        def _():
            earlier_scores(d - 1)

    @pl.when(me >= 1)
    def _():
        earlier_scores(me)

    row_max = jnp.max(mbuf[...], axis=-1, keepdims=True)
    mbuf[...] = jnp.broadcast_to(row_max, mbuf.shape)
    e0 = jnp.exp(sbuf[0] - mbuf[...])
    lbuf[...] = e0
    acc[...] = dot(e0.astype(BF16), vbuf[0])

    @pl.loop(1, me + 1)
    def _(d):
        for j in range(1, RK):
            vforward(d, j, lax.rem(rep + j, R)).wait_recv()
        ex = jnp.exp(sbuf[d] - mbuf[...])
        lbuf[...] = lbuf[...] + ex
        acc[...] = acc[...] + dot(ex.astype(BF16), vbuf[d])

    sq = jnp.zeros((T, HEAD_SIZE), F32)
    for h in range(H):
        rows = slice(h * T, (h + 1) * T)
        cols = slice(h * HEAD_SIZE, (h + 1) * HEAD_SIZE)
        total = jnp.sum(lbuf[rows, :], axis=-1, keepdims=True)
        hv = stream_ref[:, cols].astype(F32) + acc[rows, :] / total
        hid[:, cols] = hv
        sq = sq + hv * hv
    ssbuf[f] = jnp.broadcast_to(to_row(jnp.sum(sq, axis=-1, keepdims=True)), (8, T))

    def sscopy(j, owner):
        return rc(ssbuf.at[owner], ssbuf.at[owner], ss_send.at[j], ss_recv.at[owner], feat_dev(j))

    def lgcopy(j, owner):
        return rc(lgbuf.at[owner], lgbuf.at[owner], lg_send.at[j], lg_recv.at[owner], feat_dev(j))

    for j in range(1, F):
        sscopy(j, f).start()
    gain = gain_ref[...].astype(F32).reshape(1, W)
    nrm[...] = (hid[...] * gain).astype(BF16)

    def dcopy(d):
        return rc(dsrc.at[d], dbuf.at[d], d_send.at[d], d_recv.at[d], ctx_dev(d))

    def gathered(d):
        return lax.dot_general(
            place[d], nrm[...], (((0,), (0,)), ((), ())), preferred_element_type=F32
        ).astype(BF16)

    @pl.loop(1, C)
    def _(d):
        dsrc[d] = gathered(d)
        dcopy(d).start()

    dbuf[0] = gathered(0)

    for c in weights:
        c.wait()

    def rep_at(j):
        return lax.rem(rep + j, R)

    def sec_at(j):
        return lax.rem(sec + j, S)

    def acopy(d, j, owner):
        return rc(
            asrc.at[d, rep_at(j)], abuf.at[d, owner], a_send.at[d, j], a_recv.at[d, owner],
            {"rep": rep_at(j)},
        )

    def bcopy(d, j, owner):
        return rc(
            bsrc.at[d], bbuf.at[d, owner], b_send.at[d, j], b_recv.at[d, owner],
            {"section": sec_at(j)},
        )

    def icopy(d, j, owner):
        return rc(
            ibuf.at[d, owner], ibuf.at[d, owner], i_send.at[d, j], i_recv.at[d, owner],
            {"rep": rep_at(j)},
        )

    def ycopy(d):
        return rc(ysrc.at[d], ybuf.at[d], y_send.at[d], y_recv.at[d], ctx_dev(-d))

    def stage_g(d):
        x = dbuf[d]
        for r in range(R):
            cols = slice(r * HR, (r + 1) * HR)
            asrc[d, r, :, 0:HR] = dot(x, wg[:, cols]).astype(BF16)
            asrc[d, r, :, HR : 2 * HR] = dot(x, wu[:, cols]).astype(BF16)
        for j in range(1, R):
            acopy(d, j, rep).start()

    def stage_b(d):
        total = asrc[d, rep].astype(F32)
        for j in range(1, R):
            acopy(d, j, rep_at(j)).wait_recv()
            total = total + abuf[d, rep_at(j)].astype(F32)
        bsrc[d] = total.astype(BF16)
        for j in range(1, S):
            bcopy(d, j, sec).start()

    eye_cap = lax.broadcasted_iota(jnp.int32, (cap, cap), 0) == lax.broadcasted_iota(
        jnp.int32, (cap, cap), 1
    )

    def ccopy(d):
        return rc(scsrc.at[d], scbuf.at[d], c_send.at[d], c_recv.at[d], ctx_dev(d))

    def rows_scale(d):
        return jnp.sum(jnp.where(eye_cap, scbuf[d, 0:1, 0:cap], 0.0), axis=1, keepdims=True)

    def stage_i(d):
        total = bsrc[d].astype(F32)
        for j in range(1, S):
            bcopy(d, j, sec_at(j)).wait_recv()
            total = total + bbuf[d, sec_at(j)].astype(F32)
        total = total * rows_scale(d)
        g = total[:, 0:HR]
        u = total[:, HR : 2 * HR]
        ibuf[d, rep] = (g * jax.nn.sigmoid(g) * u).astype(BF16)
        for j in range(1, R):
            icopy(d, j, rep).start()

    def stage_d(d):
        for j in range(1, R):
            icopy(d, j, rep_at(j)).wait_recv()
        y = dot(ibuf[d, 0], wd[0:HR, :])
        for r in range(1, R):
            y = y + dot(ibuf[d, r], wd[r * HR : (r + 1) * HR, :])
        return y.astype(BF16)

    stage_g(0)

    for j in range(1, F):
        sscopy(j, feat(j)).wait_recv()
    ss = ssbuf[0]
    for g in range(1, F):
        ss = ss + ssbuf[g]
    scale_rows = lax.rsqrt(to_col(ss[0:1, :]) / (W * F) + epsilon)

    def slot_scale(d):
        return jnp.sum(jnp.where(place[d].astype(F32) > 0.5, scale_rows, 0.0), axis=0, keepdims=True)

    @pl.loop(1, C)
    def _(d):
        scsrc[d, 0:1, 0:cap] = slot_scale(d)
        ccopy(d).start()

    scbuf[0, 0:1, 0:cap] = slot_scale(0)

    stage_b(0)

    normed = (hid[...] * scale_rows * gain).astype(BF16)
    lgbuf[f, 0:E, :] = lax.dot_general(
        router_ref[...], normed, (((1,), (1,)), ((), ())), preferred_element_type=F32
    )
    for j in range(1, F):
        lgcopy(j, f).start()

    if C > 1:
        dcopy(1).wait_recv()
        stage_g(1)
    stage_i(0)
    if C > 1:
        stage_b(1)
    ybuf[0] = stage_d(0)

    @pl.loop(2, C)
    def _(d):
        dcopy(d).wait_recv()
        stage_g(d)
        ccopy(d - 1).wait_recv()
        stage_i(d - 1)
        stage_b(d)
        ysrc[d - 1] = stage_d(d - 1)
        ycopy(d - 1).start()

    if C > 1:
        ccopy(C - 1).wait_recv()
        stage_i(C - 1)
        ysrc[C - 1] = stage_d(C - 1)
        ycopy(C - 1).start()

    for j in range(1, F):
        lgcopy(j, feat(j)).wait_recv()
    lt = lgbuf[0]
    for g in range(1, F):
        lt = lt + lgbuf[g]
    picked = jnp.zeros(ids.shape, F32)
    for e in range(E):
        picked = jnp.where(ids == e, lt[e : e + 1, :], picked)
    squashed = jax.nn.sigmoid(picked)
    gates = squashed / jnp.sum(squashed, axis=0, keepdims=True)
    gate_cols = [to_col(gates[k : k + 1, :]) for k in range(top)]

    def weighted(d):
        gd = jnp.zeros((T, 1), F32)
        for k in range(top):
            gd = gd + jnp.where(rel_cols[k] == d, gate_cols[k], 0.0)
        return gd * dot(place[d], ybuf[d])

    hid[...] = hid[...] + weighted(0)

    @pl.loop(1, C)
    def _(d):
        ycopy(d).wait_recv()
        hid[...] = hid[...] + weighted(d)

    out_ref[...] = hid[...]

    @pl.loop(1, C - me)
    def _(d):
        kcopy(d).wait_send()
        vcopy(d).wait_send()

    @pl.loop(1, me + 1)
    def _(d):
        for j in range(1, RK):
            kforward(d, j, rep).wait_send()
            vforward(d, j, rep).wait_send()

    for j in range(1, F):
        sscopy(j, f).wait_send()
        lgcopy(j, f).wait_send()

    @pl.loop(0, C)
    def _(d):
        for j in range(1, R):
            acopy(d, j, rep).wait_send()
            icopy(d, j, rep).wait_send()
        for j in range(1, S):
            bcopy(d, j, sec).wait_send()

    @pl.loop(1, C)
    def _(d):
        dcopy(d).wait_send()
        ccopy(d).wait_send()
        ycopy(d).wait_send()


def local(C, S, R, stream, q, k, v, ids, home, router, gain, w_gate, w_up, w_down):
    T, W = stream.shape
    top = ids.shape[1]
    H = W // HEAD_SIZE
    F = S * R
    E = router.shape[1]
    HID = w_gate.shape[2]
    HR = HID // R
    capacity = min(T, max(2, 5 * T * top // (4 * C)))
    cap = -(-capacity // 16) * 16
    e_rows = -(-E // 8) * 8
    lanes = -(-cap // 128) * 128
    DMA = pltpu.SemaphoreType.DMA
    vmem = pl.BlockSpec(memory_space=pltpu.VMEM)
    smem = pl.BlockSpec(memory_space=pltpu.SMEM)
    hbm = pl.BlockSpec(memory_space=pltpu.HBM)
    V = pltpu.VMEM
    scratch = [
        V((T, W), BF16), V((T, W), BF16), V(k.shape, BF16), V(k.shape, BF16),
        V((top, T), jnp.int32), V((E, W), BF16), V((W,), BF16),
        V((W, HID), BF16), V((W, HID), BF16), V((HID, W), BF16),
        V((H * T, HEAD_SIZE), BF16),
        V((C, T, HEAD_SIZE), BF16), V((C, T, HEAD_SIZE), BF16),
        V((C, H * T, T), F32), V((H * T, T), F32), V((H * T, T), F32),
        V((H * T, HEAD_SIZE), F32),
        V((T, W), F32), V((T, W), BF16),
        V((F, 8, T), F32), V((F, e_rows, T), F32),
        V((C, T, cap), BF16), V((C, 8, lanes), F32), V((C, 8, lanes), F32),
        V((C, cap, W), BF16), V((C, cap, W), BF16),
        V((C, R, cap, 2 * HR), BF16), V((C, R, cap, 2 * HR), BF16),
        V((C, cap, 2 * HR), BF16), V((C, S, cap, 2 * HR), BF16),
        V((C, R, cap, HR), BF16),
        V((C, cap, W), BF16), V((C, cap, W), BF16),
        DMA((3,)), DMA((7,)), DMA((C, R)), DMA((C, R)), DMA((C, R)), DMA((C, R)), DMA((C,)), DMA((C,)),
        DMA((C,)), DMA((C,)), DMA((C,)), DMA((C,)),
        DMA((F,)), DMA((F,)), DMA((F,)), DMA((F,)),
        DMA((C,)), DMA((C,)),
        DMA((C, R)), DMA((C, R)),
        DMA((C, S)), DMA((C, S)),
        DMA((C, R)), DMA((C, R)),
        DMA((C,)), DMA((C,)),
    ]
    used = sum(
        math.prod(x.shape) * jnp.dtype(x.dtype).itemsize for x in scratch if x.dtype in (F32, BF16)
    )
    limit = 62 << 20
    return pl.pallas_call(
        functools.partial(body, C, S, R, cap),
        out_shape=jax.ShapeDtypeStruct((T, W), F32),
        in_specs=[hbm] * 5 + [smem] + [hbm] * 5,
        out_specs=vmem,
        scratch_shapes=scratch,
        compiler_params=pltpu.CompilerParams(
            collective_id=0, has_side_effects=True, vmem_limit_bytes=limit
        ),
        name="block",
    )(stream, q, k, v, ids.T, home, router.T, gain, w_gate, w_up, w_down).astype(BF16)


def solution(mesh):
    placed = (
        P(("group", "ctx"), ("section", "rep")),
        P(("group", "ctx"), ("section", "rep")),
        P(("group", "ctx"), None),
        P(("group", "ctx"), None),
        P(("group", "ctx"), None),
        P(),
        P(("section", "rep"), None),
        P(("section", "rep")),
        P("ctx", ("section", "rep"), None),
        P("ctx", ("section", "rep"), None),
        P("ctx", None, ("section", "rep")),
    )
    return jax.shard_map(
        functools.partial(
            local, mesh.shape["ctx"], mesh.shape["section"], mesh.shape["rep"]
        ),
        mesh=mesh,
        in_specs=placed,
        out_specs=P(("group", "ctx"), ("section", "rep")),
        check_vma=False,
    )
```
